32 devices in a mesh: half: 2 (over core), grp: 16 (over z, y, x).
Axes of the slice: x: 2, y: 2, z: 4, core: 2. Of those that a mesh axis runs over, the one named last changes fastest.
Arguments:
- weights: float32 [2, 16, 2, 8192, 128], P('half', 'grp'), may hold values from -4 to 4
- accum: float32 [2, 16, 2, 8192], P('half', 'grp'), may hold values from 0.01 to 1
- grads: float32 [32, 32, 16, 128], P(('half', 'grp')), may hold values from -6 to 6
- row_ids: int32 [32, 32, 16], P(('half', 'grp')), may hold values from 0 to 16383
- counts: int32 [32, 32], P(('half', 'grp')), may hold values from 1 to 16, as said below
Outputs:
- new_weights: float32 [2, 16, 2, 8192, 128], P('half', 'grp')
- new_accum: float32 [2, 16, 2, 8192], P('half', 'grp')
The draws below stay inside these ranges and needn't reach their ends.
Inputs may be any that keep to these rules, and one draw needn't show every extreme that they name: `counts`: A few owners, the same for all senders, receive 16 live rows from every sender; no two of them share a shard index g (owners g and 16 + g). The owner that shares its shard index with such an owner receives 16 // 2 live rows from every sender; each other count lies from 1 to 8. So the two owners of one shard index receive at most 24 live rows from one sender together, and some pair receives exactly that.
All inputs are finite; a program needn't handle non-finite values.
Results may differ from the reference program's by a relative error of at most 0.00002.
Values sent between devices are 32-bit elements; how exact they have to be, the bound alone decides.
A program may use at most 128 MiB of HBM per device.

```python
import math
import jax
import jax.numpy as jnp
import numpy as np
from jax import lax

E = 128
HR = 8192
SLOTS = 16
N_GRP = 16
DEVICES = 32


heavy_owners = 8


def draw_counts(key, part):
    first, second, third = jax.random.split(jax.random.fold_in(key, 11), 3)
    groups = DEVICES // 2
    base = jax.random.randint(first, (DEVICES, DEVICES), 1, SLOTS // 2 + 1)
    ranked = jax.random.permutation(second, groups)
    heavy_group = ranked < heavy_owners
    heavy_bit = jax.random.randint(third, (groups,), 0, 2)
    owner = jnp.arange(DEVICES, dtype=jnp.int32)
    owner_half = owner // groups
    owner_group = owner % groups
    in_heavy = heavy_group[owner_group]
    heavy = in_heavy & (owner_half == heavy_bit[owner_group])
    partner = in_heavy & jnp.logical_not(heavy)
    result = jnp.where(heavy[None, :], SLOTS, jnp.where(partner[None, :], SLOTS // 2, base))
    return result.astype(jnp.int32)


def place_ends(values, stream_key, low, largest):
    longest = values.shape.index(max(values.shape))
    spots = []
    for shift in (0, 1):
        where = [jax.random.randint(jax.random.fold_in(stream_key, axis), (), 0, length) for axis, length in enumerate(values.shape)]
        where[longest] = (where[longest] + shift) % values.shape[longest]
        spots.append(tuple(where))
    return values.at[spots[0]].set(low).at[spots[1]].set(largest)


def raised(values, key, source, target, blocks, factor):
    owner, partner = [(jnp.arange(values.shape[position]) // (values.shape[position] // blocks)).reshape([-1 if axis == position else 1 for axis in range(values.ndim)]) for position in (source, target)]
    chosen = jax.random.permutation(key, blocks)[partner]
    strong = (owner == chosen) | (owner == (partner + blocks // 2) % blocks)
    return jnp.where(strong, factor * values, values)


def block_scale(rng, dims, pieces, low, high):
    def one(axis_at, parts):
        steps = jax.random.uniform(jax.random.fold_in(jax.random.fold_in(rng, 6), axis_at), (parts,), jnp.float32, low / len(pieces), high / len(pieces))
        return jnp.repeat(jnp.exp(steps), dims[axis_at] // parts).reshape((-1,) + (1,) * (len(dims) - axis_at - 1))

    factor_of = one(*pieces[0])
    for cut in pieces[1:]:
        factor_of = factor_of * one(*cut)
    return factor_of


def rank_bounds(number_of, lean):
    loads = [(1 << 20) // math.isqrt(rank ** lean) + 1 for rank in range(1, number_of + 1)]
    spread = 1 + sum(loads) // (1 << 30)
    return np.cumsum(np.array([max(1, weight // spread) for weight in loads]))


def ranked_ids(stream_key, dims, number_of, slope):
    grid = rank_bounds(number_of, slope)
    pick = jax.random.randint(jax.random.fold_in(stream_key, 1), dims, 0, int(grid[number_of - 1]))
    standing = jnp.searchsorted(jnp.asarray(grid, jnp.int32), pick, side="right")
    return jax.random.permutation(jax.random.fold_in(stream_key, 2), number_of)[standing].astype(jnp.int32)


def noise(own_key, shape, deviation, most, shards=(), kind=jnp.bfloat16):
    drawn = deviation * jax.random.normal(own_key, shape, jnp.float32)
    if shards:
        drawn = drawn * block_scale(own_key, shape, shards, -0.22, 0.18)
    return jnp.clip(drawn, -most, most).astype(kind)


def bell_draw_with(stream_key, extent, width, limit, cuts, heavy, kind=jnp.bfloat16):
    values = width * jax.random.normal(stream_key, extent, jnp.float32)
    if cuts:
        values = values * block_scale(stream_key, extent, cuts, -0.22, 0.18)
    return jnp.clip(raised(values, jax.random.fold_in(stream_key, 3), *heavy), -limit, limit).astype(kind)


def setup_inputs(seed: int = 0) -> dict:
    seeds = jax.random.split(jax.random.key(seed), 6)
    weights = noise(seeds[0], (2, N_GRP, 2, HR, E), 0.5, 4.0, ((0, 2), (1, 16)), jnp.float32)
    accum = jnp.clip(jnp.exp(math.log(1.0) - 4.6051702 * jax.random.uniform(seeds[1], (2, N_GRP, 2, HR), jnp.float32) ** block_scale(seeds[1], (2, N_GRP, 2, HR), ((0, 2), (1, 16)), -0.2, 0.2)), 0.01, 1.0)
    grads = bell_draw_with(seeds[2], (DEVICES, DEVICES, SLOTS, E), 1.0, 6.0, ((0, 32),), (0, 1, 32, 2.75), jnp.float32)
    row_ids = place_ends(ranked_ids(seeds[3], (DEVICES, DEVICES, SLOTS), 2 * HR, 2), jax.random.fold_in(seeds[3], 3), 0, (2 * HR) - 1).astype(jnp.int32)
    counts = draw_counts(jax.random.fold_in(seeds[5], 71), 0)
    return {"weights": weights, "accum": accum, "grads": grads, "row_ids": row_ids, "counts": counts}


LEARN_RATE = 0.5
EPSILON = 1e-06

def reference(weights, accum, grads, row_ids, counts):
    groups = N_GRP
    owners = 2 * groups
    moved = jnp.transpose(weights, (2, 1, 0, 3, 4)).reshape(owners, 2 * HR, E)
    moved_acc = jnp.transpose(accum, (2, 1, 0, 3)).reshape(owners, 2 * HR)
    slot_index = lax.broadcasted_iota(jnp.int32, (owners, owners, SLOTS), 2)
    live = slot_index < counts[:, :, None]
    masked = jnp.where(live[..., None], grads, jnp.zeros_like(grads))
    owner_index = lax.broadcasted_iota(jnp.int32, (owners, owners, SLOTS), 1)
    flat_rows = (owner_index * (2 * HR) + row_ids.astype(jnp.int32)).reshape(-1)
    total = jnp.zeros((owners * 2 * HR, E), jnp.float32).at[flat_rows].add(masked.reshape(-1, E))
    total = total.reshape(owners, 2 * HR, E)
    accumulated = moved_acc + lax.optimization_barrier(jnp.mean(total * total, axis=-1))
    updated = moved - LEARN_RATE * total / (jnp.sqrt(accumulated)[..., None] + EPSILON)
    return (updated.reshape(2, groups, 2, HR, E), accumulated.reshape(2, groups, 2, HR))
```

```python
import functools

import jax
import jax.numpy as jnp
from jax import lax
from jax.experimental import pallas as pl
from jax.experimental.pallas import tpu as pltpu
from jax.sharding import PartitionSpec as P

LEARN_RATE = 0.5
EPSILON = 1e-06
LANES = 128
MESH = pl.DeviceIdType.MESH
PIECES = 4


def exchange_kernel(
    halves, groups, weights, accum, grads, ids_t, counts,
    table, pair_acc, got, got_ids,
    block_buf, id_in, count_in, id_pad, id_buf,
    local_sem, row_send, row_recv, acc_send, acc_recv, block_send, block_recv, id_send, id_recv, ready,
):
    half = lax.axis_index("half")
    group = lax.axis_index("grp")
    owners = halves * groups
    me = half * groups + group
    other = 1 - half
    slots = ids_t.shape[0]
    rows_half = weights.shape[1]
    piece = rows_half // PIECES
    home = pl.multiple_of(half * rows_half, rows_half)

    barrier = pltpu.get_barrier_semaphore()
    pl.semaphore_signal(barrier, inc=1, device_id=(other, group), device_id_type=MESH)
    id_load = pltpu.make_async_copy(ids_t, id_in, local_sem.at[1])
    count_load = pltpu.make_async_copy(counts, count_in, local_sem.at[2])
    load = pltpu.make_async_copy(grads, block_buf, local_sem.at[0])
    keep = pltpu.make_async_copy(
        weights.at[half], table.at[pl.ds(home, rows_half)], local_sem.at[3])
    keep_acc = pltpu.make_async_copy(accum, pair_acc.at[half], local_sem.at[4])
    id_load.start()
    count_load.start()
    load.start()

    @pl.loop(group + 1, groups)
    def _(peer_group):
        for peer_half in range(halves):
            pl.semaphore_signal(barrier, inc=1, device_id=(peer_half, peer_group), device_id_type=MESH)

    id_load.wait()
    count_load.wait()
    slot = lax.broadcasted_iota(jnp.int32, ids_t.shape, 0)
    id_pad[...] = jnp.full(id_pad.shape, -1, jnp.int32)
    id_pad[0:slots, 0:owners] = jnp.where(slot < count_in[...], id_in[...], -1)
    turned = id_pad[...].T
    for owner in range(owners):
        id_buf[owner, 0:1, :] = turned[owner:owner + 1, :]
    pl.semaphore_wait(barrier, halves * group + 1)

    @pl.loop(0, group)
    def _(peer_group):
        for peer_half in range(halves):
            pl.semaphore_signal(
                ready.at[group], inc=1, device_id=(peer_half, peer_group), device_id_type=MESH)

    def block_copy(peer_half, peer_group, lands=None):
        peer = peer_half * groups + peer_group
        at = me if lands is None else peer
        return pltpu.make_async_remote_copy(
            src_ref=block_buf.at[peer], dst_ref=got.at[at],
            send_sem=block_send.at[peer], recv_sem=block_recv.at[at],
            device_id=(peer_half, peer_group), device_id_type=MESH)

    def id_copy(peer_half, peer_group, lands=None):
        peer = peer_half * groups + peer_group
        at = me if lands is None else peer
        return pltpu.make_async_remote_copy(
            src_ref=id_buf.at[peer], dst_ref=got_ids.at[at],
            send_sem=id_send.at[peer], recv_sem=id_recv.at[at],
            device_id=(peer_half, peer_group), device_id_type=MESH)

    def row_copy(index):
        rows = pl.ds(index * piece, piece)
        return pltpu.make_async_remote_copy(
            src_ref=weights.at[other, rows],
            dst_ref=table.at[pl.ds(pl.multiple_of(home + index * piece, piece), piece)],
            send_sem=row_send.at[index], recv_sem=row_recv.at[index],
            device_id=(other, group), device_id_type=MESH)

    acc_copy = pltpu.make_async_remote_copy(
        src_ref=accum, dst_ref=pair_acc.at[half], send_sem=acc_send, recv_sem=acc_recv,
        device_id=(other, group), device_id_type=MESH)
    acc_copy.start()
    for index in range(PIECES):
        row_copy(index).start()

    @pl.loop(0, group)
    def _(peer_group):
        for peer_half in range(halves):
            id_copy(peer_half, peer_group).start()

    load.wait()

    @pl.loop(0, group)
    def _(peer_group):
        for peer_half in range(halves):
            block_copy(peer_half, peer_group).start()

    id_copy(other, group).start()
    block_copy(other, group).start()
    keep.start()
    keep_acc.start()
    own_block = pltpu.make_async_copy(block_buf.at[me], got.at[me], local_sem.at[0])
    own_ids = pltpu.make_async_copy(id_buf.at[me], got_ids.at[me], local_sem.at[1])
    own_block.start()
    own_ids.start()

    @pl.loop(group + 1, groups)
    def _(peer_group):
        pl.semaphore_wait(ready.at[peer_group], halves)
        for peer_half in range(halves):
            id_copy(peer_half, peer_group).start()
            block_copy(peer_half, peer_group).start()

    own_block.wait()
    own_ids.wait()

    def finish(peer_half, peer_group):
        id_copy(peer_half, peer_group).wait_send()
        block_copy(peer_half, peer_group).wait_send()
        id_copy(peer_half, peer_group, "here").wait_recv()
        block_copy(peer_half, peer_group, "here").wait_recv()

    finish(other, group)

    @pl.loop(1, groups)
    def _(step):
        peer_group = lax.rem(group + step, groups)
        for peer_half in range(halves):
            finish(peer_half, peer_group)

    acc_copy.wait()
    for index in range(PIECES):
        row_copy(index).wait()
    keep.wait()
    keep_acc.wait()


def thirds(value):
    first = value.astype(jnp.bfloat16)
    rest = value - first.astype(jnp.float32)
    second = rest.astype(jnp.bfloat16)
    third = (rest - second.astype(jnp.float32)).astype(jnp.bfloat16)
    return jnp.concatenate([first, second, third], axis=1)


def joined(value, width):
    return value[:, 0:width] + value[:, width:2 * width] + value[:, 2 * width:3 * width]


def update_kernel(
    table_in, pair_acc, got, got_ids, table, new_weights, new_accum,
    out_acc, state, id_list, picked, delta, in_sem, out_sem, id_sem,
):
    half = lax.axis_index("half")
    senders, slots, width = got.shape
    count = senders * slots
    rows_half = pair_acc.shape[2]
    piece = rows_half // PIECES
    spare = 2 * rows_half
    acc_rows = rows_half // LANES

    ids_in = pltpu.make_async_copy(got_ids, id_list, id_sem)
    ids_in.start()
    table[spare:spare + 8, :] = jnp.zeros((8, width), jnp.float32)

    is_low = half == 0
    for old in range(2):
        line = jnp.where(is_low, pair_acc[old, 0:1, :], pair_acc[old, 1:2, :])
        for row in range(acc_rows):
            at = old * acc_rows + row
            state[at:at + 1, :] = line[:, row * LANES:(row + 1) * LANES]

    lane = lax.broadcasted_iota(jnp.int32, (count, LANES), 1)
    sub = lax.broadcasted_iota(jnp.int32, (count, LANES), 0)
    spread = jnp.broadcast_to(got_ids[...], (senders, slots, LANES)).reshape(count, LANES)
    mine = jnp.where(lane == lax.rem(sub, slots), spread, 0).astype(jnp.float32)
    column = jnp.sum(mine, axis=1, keepdims=True)
    wide = jnp.broadcast_to(column, (count, LANES))
    line = wide.T[0:1, :]
    grad_parts = thirds(got[...].reshape(count, width))
    old_state = state[...]
    state_parts = thirds(old_state)
    lane_f = lane.astype(jnp.float32)
    block = min(count, 512)
    gain = jnp.zeros((2 * acc_rows, 3 * LANES), jnp.float32)
    high_line = jnp.floor(line * (1.0 / LANES))
    for start in range(0, count, block):
        key = column[start:start + block]
        same = key == line
        hot = jnp.where(same, 1.0, 0.0)
        total = joined(jnp.dot(hot.astype(jnp.bfloat16), grad_parts,
                               preferred_element_type=jnp.float32), width)
        at_col = lax.broadcasted_iota(jnp.int32, (block, count), 1)
        at_row = lax.broadcasted_iota(jnp.int32, (block, count), 0) + start
        earlier = jnp.sum(jnp.where(at_col < at_row, hot, 0.0), axis=1, keepdims=True)
        high = jnp.floor(key * (1.0 / LANES))
        low = key - high * LANES
        row_hot = jnp.where(lane_f[:block] == high, 1.0, 0.0).astype(jnp.bfloat16) if acc_rows * 2 == LANES else jnp.where(
            lax.broadcasted_iota(jnp.int32, (block, 2 * acc_rows), 1).astype(jnp.float32) == high, 1.0, 0.0).astype(jnp.bfloat16)
        state_rows = joined(jnp.dot(row_hot, state_parts, preferred_element_type=jnp.float32), LANES)
        at_low = lane_f[:block] == low
        old_acc = jnp.sum(jnp.where(at_low, state_rows, 0.0), axis=1, keepdims=True)
        square = jnp.sum(total * total, axis=1, keepdims=True) * (1.0 / width)
        delta[start:start + block, :] = LEARN_RATE * total / (jnp.sqrt(old_acc + square) + EPSILON)
        once = jnp.where((earlier == 0.0) & (key >= 0.0), square, 0.0)
        add_parts = thirds(jnp.where(at_low, once, 0.0))
        high_of = high_line[:, start:start + block]
        tall = lax.broadcasted_iota(jnp.int32, (2 * acc_rows, block), 0).astype(jnp.float32)
        tall_hot = jnp.where(tall == high_of, 1.0, 0.0).astype(jnp.bfloat16)
        gain = gain + jnp.dot(tall_hot, add_parts, preferred_element_type=jnp.float32)
    state[...] = old_state + joined(gain, LANES)
    for old in range(2):
        for row in range(acc_rows):
            at = old * acc_rows + row
            out_acc[old:old + 1, row * LANES:(row + 1) * LANES] = state[at:at + 1, :]

    acc_out = pltpu.make_async_copy(out_acc, new_accum, in_sem)
    acc_out.start()
    ids_in.wait()

    def place(sender, slot):
        at = id_list[sender, 0, slot]
        return jnp.where(at < 0, spare, at)

    @pl.loop(0, senders)
    def _(sender):
        base = pl.multiple_of(sender * slots, slots)
        rows = [table[pl.ds(place(sender, slot), 1), :] for slot in range(slots)]
        for slot in range(slots):
            picked[pl.ds(base + slot, 1), :] = rows[slot]

    picked[...] = picked[...] - delta[...]

    @pl.loop(0, senders)
    def _(sender):
        base = pl.multiple_of(sender * slots, slots)
        rows = [picked[pl.ds(base + slot, 1), :] for slot in range(slots)]
        for slot in range(slots):
            table[pl.ds(place(sender, slot), 1), :] = rows[slot]

    stores = []
    for old in range(2):
        for index in range(PIECES):
            stores.append(pltpu.make_async_copy(
                table.at[pl.ds(old * rows_half + index * piece, piece)],
                new_weights.at[old, pl.ds(index * piece, piece)],
                out_sem.at[old * PIECES + index]))
    for store in stores:
        store.start()
    for store in stores:
        store.wait()
    acc_out.wait()


def per_device(halves, groups, weights, accum, grads, row_ids, counts):
    owners, slots, width = grads.shape[1:]
    rows_half = weights.shape[3]
    table = weights[0, 0]
    state = accum[0, 0]
    count = owners * slots
    hbm = pl.BlockSpec(memory_space=pltpu.HBM)
    vmem = pl.BlockSpec(memory_space=pltpu.VMEM)
    id_width = -(-owners // LANES) * LANES
    dma = pltpu.SemaphoreType.DMA
    landed = (
        jax.ShapeDtypeStruct((2 * rows_half + 8, width), jnp.float32),
        jax.ShapeDtypeStruct((2, 2, rows_half), jnp.float32),
        jax.ShapeDtypeStruct((owners, slots, width), jnp.float32),
        jax.ShapeDtypeStruct((owners, 1, LANES), jnp.int32),
    )
    moved, pair_acc, got, got_ids = pl.pallas_call(
        functools.partial(exchange_kernel, halves, groups),
        out_shape=landed,
        in_specs=[hbm] * 5,
        out_specs=(vmem,) * 4,
        scratch_shapes=[
            pltpu.VMEM((owners, slots, width), jnp.float32),
            pltpu.VMEM((slots, owners), jnp.int32),
            pltpu.VMEM((1, owners), jnp.int32),
            pltpu.VMEM((LANES, id_width), jnp.int32),
            pltpu.VMEM((owners, 1, LANES), jnp.int32),
            dma((5,)),
            dma((PIECES,)), dma((PIECES,)),
            dma, dma,
            dma((owners,)), dma((owners,)),
            dma((owners,)), dma((owners,)),
            pltpu.SemaphoreType.REGULAR((groups,)),
        ],
        compiler_params=pltpu.CompilerParams(
            collective_id=0, has_side_effects=True, vmem_limit_bytes=16 << 20),
        name="exchange",
    )(*(pltpu.with_memory_space_constraint(value, pltpu.HBM)
        for value in (table, state, grads[0], row_ids[0].T, counts)))
    _, new_weights, new_accum = pl.pallas_call(
        update_kernel,
        out_shape=(
            jax.ShapeDtypeStruct((2 * rows_half + 8, width), jnp.float32),
            jax.ShapeDtypeStruct((2, rows_half, width), jnp.float32),
            jax.ShapeDtypeStruct((2, rows_half), jnp.float32),
        ),
        in_specs=[vmem] * 4,
        out_specs=(vmem, hbm, hbm),
        scratch_shapes=[
            pltpu.VMEM((2, rows_half), jnp.float32),
            pltpu.VMEM((2 * rows_half // LANES, LANES), jnp.float32),
            pltpu.SMEM((owners, 1, LANES), jnp.int32),
            pltpu.VMEM((count, width), jnp.float32),
            pltpu.VMEM((count, width), jnp.float32),
            dma, dma((2 * PIECES,)), dma,
        ],
        input_output_aliases={0: 0},
        compiler_params=pltpu.CompilerParams(vmem_limit_bytes=32 << 20),
        name="update",
    )(moved, pair_acc, got, got_ids)
    return new_weights[None, None], new_accum[None, None]


def solution(mesh):
    placed = (
        P("half", "grp", None, None, None),
        P("half", "grp", None, None),
        P(("half", "grp"), None, None, None),
        P(("half", "grp"), None, None),
        P(("half", "grp"), None),
    )
    return jax.shard_map(
        functools.partial(per_device, mesh.shape["half"], mesh.shape["grp"]),
        mesh=mesh,
        in_specs=placed,
        out_specs=(P("half", "grp", None, None, None), P("half", "grp", None, None)),
        check_vma=False,
    )
```

```python
import functools
import math

import jax
import jax.numpy as jnp
from jax import lax
from jax.experimental import pallas as pl
from jax.experimental.pallas import tpu as pltpu
from jax.sharding import PartitionSpec as P

LEARN_RATE = 0.5
EPSILON = 1e-06
LANES = 128
MESH = pl.DeviceIdType.MESH
PIECES = 4


def axes_of(groups):
    first = 4 if groups % 4 == 0 else groups
    rest = groups // first
    side = math.isqrt(rest)
    return (first, side, side) if side * side == rest else (first, rest, 1)


def exchange_kernel(
    halves, groups, weights, accum, grads, ids_t, counts,
    table, pair_acc, got, got_ids,
    block_buf, id_in, count_in, id_pad, id_buf,
    local_sem, row_send, row_recv, acc_send, acc_recv, block_send, block_recv, id_send, id_recv, ready,
):
    half = lax.axis_index("half")
    group = lax.axis_index("grp")
    owners = halves * groups
    me = half * groups + group
    other = 1 - half
    slots = ids_t.shape[0]
    rows_half = weights.shape[1]
    piece = rows_half // PIECES
    home = pl.multiple_of(half * rows_half, rows_half)

    size_a, size_b, size_c = axes_of(groups)
    at_a = group // (size_b * size_c)
    at_b = lax.rem(group // size_c, size_b)
    at_c = lax.rem(group, size_c)

    def box(low, high, act):
        @pl.loop(low[0], high[0])
        def _(a):
            @pl.loop(low[1], high[1])
            def _(b):
                @pl.loop(low[2], high[2])
                def _(c):
                    peer_group = (a * size_b + b) * size_c + c

                    @pl.when(peer_group != group)
                    def _():
                        act(peer_group, (a, b, c))

    here = (at_a, at_b, at_c)
    past = (at_a + 1, at_b + 1, at_c + 1)

    def descendants(act):
        box(here, (size_a, size_b, size_c), act)

    def ancestors(act):
        box((0, 0, 0), past, act)

    barrier = pltpu.get_barrier_semaphore()
    pl.semaphore_signal(barrier, inc=1, device_id=(other, group), device_id_type=MESH)
    id_load = pltpu.make_async_copy(ids_t, id_in, local_sem.at[1])
    count_load = pltpu.make_async_copy(counts, count_in, local_sem.at[2])
    load = pltpu.make_async_copy(grads, block_buf, local_sem.at[0])
    keep = pltpu.make_async_copy(
        weights.at[half], table.at[pl.ds(home, rows_half)], local_sem.at[3])
    keep_acc = pltpu.make_async_copy(accum, pair_acc.at[half], local_sem.at[4])
    id_load.start()
    count_load.start()
    load.start()

    def greet(peer_group, _):
        for peer_half in range(halves):
            pl.semaphore_signal(barrier, inc=1, device_id=(peer_half, peer_group), device_id_type=MESH)

    descendants(greet)
    id_load.wait()
    count_load.wait()
    slot = lax.broadcasted_iota(jnp.int32, ids_t.shape, 0)
    id_pad[...] = jnp.full(id_pad.shape, -1, jnp.int32)
    id_pad[0:slots, 0:owners] = jnp.where(slot < count_in[...], id_in[...], -1)
    turned = id_pad[...].T
    for owner in range(owners):
        id_buf[owner, 0:1, :] = turned[owner:owner + 1, :]
    load.wait()
    pl.semaphore_wait(barrier, halves * past[0] * past[1] * past[2] - 1)

    def announce(peer_group, _):
        for peer_half in range(halves):
            pl.semaphore_signal(
                ready.at[group], inc=1, device_id=(peer_half, peer_group), device_id_type=MESH)

    ancestors(announce)

    def block_copy(peer_half, peer_group):
        return pltpu.make_async_remote_copy(
            src_ref=block_buf.at[peer_half * groups + peer_group], dst_ref=got.at[me],
            send_sem=block_send, recv_sem=block_recv,
            device_id=(peer_half, peer_group), device_id_type=MESH)

    def id_copy(peer_half, peer_group):
        return pltpu.make_async_remote_copy(
            src_ref=id_buf.at[peer_half * groups + peer_group], dst_ref=got_ids.at[me],
            send_sem=id_send, recv_sem=id_recv,
            device_id=(peer_half, peer_group), device_id_type=MESH)

    def send_ids(peer_group, _):
        for peer_half in range(halves):
            id_copy(peer_half, peer_group).start()

    def send_block(peer_group, _):
        for peer_half in range(halves):
            block_copy(peer_half, peer_group).start()

    def row_copy(index):
        rows = pl.ds(index * piece, piece)
        return pltpu.make_async_remote_copy(
            src_ref=weights.at[other, rows],
            dst_ref=table.at[pl.ds(pl.multiple_of(home + index * piece, piece), piece)],
            send_sem=row_send.at[index], recv_sem=row_recv.at[index],
            device_id=(other, group), device_id_type=MESH)

    acc_copy = pltpu.make_async_remote_copy(
        src_ref=accum, dst_ref=pair_acc.at[half], send_sem=acc_send, recv_sem=acc_recv,
        device_id=(other, group), device_id_type=MESH)
    acc_copy.start()
    for index in range(PIECES):
        row_copy(index).start()
    ancestors(send_ids)
    ancestors(send_block)
    id_copy(other, group).start()
    block_copy(other, group).start()
    keep.start()
    keep_acc.start()

    def serve(joined_group, point):
        pl.semaphore_wait(ready.at[joined_group], halves)
        low = tuple(jnp.where(at > mine, at, 0) for at, mine in zip(point, here))
        high = tuple(at + 1 for at in point)

        def send(peer_group, _):
            send_ids(peer_group, None)
            send_block(peer_group, None)

        box(low, high, send)

    descendants(serve)
    got[me] = block_buf[me]
    got_ids[me] = id_buf[me]

    def take(semaphore, ref):
        pltpu.make_async_copy(ref, ref, semaphore).wait()

    blocks = block_buf.at[pl.ds(0, owners - 1)]
    lists = id_buf.at[pl.ds(0, owners - 1)]
    take(id_send, lists)
    take(block_send, blocks)
    acc_copy.wait()
    keep_acc.wait()
    for index in range(PIECES):
        row_copy(index).wait()
    keep.wait()
    take(id_recv, lists)
    take(block_recv, blocks)


def thirds(value):
    first = value.astype(jnp.bfloat16)
    rest = value - first.astype(jnp.float32)
    second = rest.astype(jnp.bfloat16)
    third = (rest - second.astype(jnp.float32)).astype(jnp.bfloat16)
    return jnp.concatenate([first, second, third], axis=1)


def joined(value, width):
    return value[:, 0:width] + value[:, width:2 * width] + value[:, 2 * width:3 * width]


def update_kernel(
    table_in, pair_acc, got, got_ids, table, new_weights, new_accum,
    out_acc, state, id_list, picked, delta, in_sem, out_sem, id_sem,
):
    half = lax.axis_index("half")
    senders, slots, width = got.shape
    count = senders * slots
    rows_half = pair_acc.shape[2]
    piece = rows_half // PIECES
    spare = 2 * rows_half
    acc_rows = rows_half // LANES

    ids_in = pltpu.make_async_copy(got_ids, id_list, id_sem)
    ids_in.start()
    table[spare:spare + 8, :] = jnp.zeros((8, width), jnp.float32)

    is_low = half == 0
    for old in range(2):
        line = jnp.where(is_low, pair_acc[old, 0:1, :], pair_acc[old, 1:2, :])
        for row in range(acc_rows):
            at = old * acc_rows + row
            state[at:at + 1, :] = line[:, row * LANES:(row + 1) * LANES]

    lane = lax.broadcasted_iota(jnp.int32, (count, LANES), 1)
    sub = lax.broadcasted_iota(jnp.int32, (count, LANES), 0)
    spread = jnp.broadcast_to(got_ids[...], (senders, slots, LANES)).reshape(count, LANES)
    mine = jnp.where(lane == lax.rem(sub, slots), spread, 0).astype(jnp.float32)
    column = jnp.sum(mine, axis=1, keepdims=True)
    wide = jnp.broadcast_to(column, (count, LANES))
    line = wide.T[0:1, :]
    grad_parts = thirds(got[...].reshape(count, width))
    old_state = state[...]
    state_parts = thirds(old_state)
    lane_f = lane.astype(jnp.float32)
    block = min(count, 512)
    gain = jnp.zeros((2 * acc_rows, 3 * LANES), jnp.float32)
    high_line = jnp.floor(line * (1.0 / LANES))
    for start in range(0, count, block):
        key = column[start:start + block]
        same = key == line
        hot = jnp.where(same, 1.0, 0.0)
        total = joined(jnp.dot(hot.astype(jnp.bfloat16), grad_parts,
                               preferred_element_type=jnp.float32), width)
        at_col = lax.broadcasted_iota(jnp.int32, (block, count), 1)
        at_row = lax.broadcasted_iota(jnp.int32, (block, count), 0) + start
        earlier = jnp.sum(jnp.where(at_col < at_row, hot, 0.0), axis=1, keepdims=True)
        high = jnp.floor(key * (1.0 / LANES))
        low = key - high * LANES
        row_hot = jnp.where(lane_f[:block] == high, 1.0, 0.0).astype(jnp.bfloat16) if acc_rows * 2 == LANES else jnp.where(
            lax.broadcasted_iota(jnp.int32, (block, 2 * acc_rows), 1).astype(jnp.float32) == high, 1.0, 0.0).astype(jnp.bfloat16)
        state_rows = joined(jnp.dot(row_hot, state_parts, preferred_element_type=jnp.float32), LANES)
        at_low = lane_f[:block] == low
        old_acc = jnp.sum(jnp.where(at_low, state_rows, 0.0), axis=1, keepdims=True)
        square = jnp.sum(total * total, axis=1, keepdims=True) * (1.0 / width)
        delta[start:start + block, :] = LEARN_RATE * total / (jnp.sqrt(old_acc + square) + EPSILON)
        once = jnp.where((earlier == 0.0) & (key >= 0.0), square, 0.0)
        add_parts = thirds(jnp.where(at_low, once, 0.0))
        high_of = high_line[:, start:start + block]
        tall = lax.broadcasted_iota(jnp.int32, (2 * acc_rows, block), 0).astype(jnp.float32)
        tall_hot = jnp.where(tall == high_of, 1.0, 0.0).astype(jnp.bfloat16)
        gain = gain + jnp.dot(tall_hot, add_parts, preferred_element_type=jnp.float32)
    state[...] = old_state + joined(gain, LANES)
    for old in range(2):
        for row in range(acc_rows):
            at = old * acc_rows + row
            out_acc[old:old + 1, row * LANES:(row + 1) * LANES] = state[at:at + 1, :]

    acc_out = pltpu.make_async_copy(out_acc, new_accum, in_sem)
    acc_out.start()
    ids_in.wait()

    def place(sender, slot):
        at = id_list[sender, 0, slot]
        return jnp.where(at < 0, spare, at)

    @pl.loop(0, senders)
    def _(sender):
        base = pl.multiple_of(sender * slots, slots)
        rows = [table[pl.ds(place(sender, slot), 1), :] for slot in range(slots)]
        for slot in range(slots):
            picked[pl.ds(base + slot, 1), :] = rows[slot]

    picked[...] = picked[...] - delta[...]

    @pl.loop(0, senders)
    def _(sender):
        base = pl.multiple_of(sender * slots, slots)
        rows = [picked[pl.ds(base + slot, 1), :] for slot in range(slots)]
        for slot in range(slots):
            table[pl.ds(place(sender, slot), 1), :] = rows[slot]

    stores = []
    for old in range(2):
        for index in range(PIECES):
            stores.append(pltpu.make_async_copy(
                table.at[pl.ds(old * rows_half + index * piece, piece)],
                new_weights.at[old, pl.ds(index * piece, piece)],
                out_sem.at[old * PIECES + index]))
    for store in stores:
        store.start()
    for store in stores:
        store.wait()
    acc_out.wait()


def per_device(halves, groups, weights, accum, grads, row_ids, counts):
    owners, slots, width = grads.shape[1:]
    rows_half = weights.shape[3]
    table = weights[0, 0]
    state = accum[0, 0]
    count = owners * slots
    hbm = pl.BlockSpec(memory_space=pltpu.HBM)
    vmem = pl.BlockSpec(memory_space=pltpu.VMEM)
    id_width = -(-owners // LANES) * LANES
    dma = pltpu.SemaphoreType.DMA
    landed = (
        jax.ShapeDtypeStruct((2 * rows_half + 8, width), jnp.float32),
        jax.ShapeDtypeStruct((2, 2, rows_half), jnp.float32),
        jax.ShapeDtypeStruct((owners, slots, width), jnp.float32),
        jax.ShapeDtypeStruct((owners, 1, LANES), jnp.int32),
    )
    moved, pair_acc, got, got_ids = pl.pallas_call(
        functools.partial(exchange_kernel, halves, groups),
        out_shape=landed,
        in_specs=[hbm] * 5,
        out_specs=(vmem,) * 4,
        scratch_shapes=[
            pltpu.VMEM((owners, slots, width), jnp.float32),
            pltpu.VMEM((slots, owners), jnp.int32),
            pltpu.VMEM((1, owners), jnp.int32),
            pltpu.VMEM((LANES, id_width), jnp.int32),
            pltpu.VMEM((owners, 1, LANES), jnp.int32),
            dma((5,)),
            dma((PIECES,)), dma((PIECES,)),
            dma, dma,
            dma, dma, dma, dma,
            pltpu.SemaphoreType.REGULAR((groups,)),
        ],
        compiler_params=pltpu.CompilerParams(
            collective_id=0, has_side_effects=True, vmem_limit_bytes=16 << 20),
        name="exchange",
    )(*(pltpu.with_memory_space_constraint(value, pltpu.HBM)
        for value in (table, state, grads[0], row_ids[0].T, counts)))
    _, new_weights, new_accum = pl.pallas_call(
        update_kernel,
        out_shape=(
            jax.ShapeDtypeStruct((2 * rows_half + 8, width), jnp.float32),
            jax.ShapeDtypeStruct((2, rows_half, width), jnp.float32),
            jax.ShapeDtypeStruct((2, rows_half), jnp.float32),
        ),
        in_specs=[vmem] * 4,
        out_specs=(vmem, hbm, hbm),
        scratch_shapes=[
            pltpu.VMEM((2, rows_half), jnp.float32),
            pltpu.VMEM((2 * rows_half // LANES, LANES), jnp.float32),
            pltpu.SMEM((owners, 1, LANES), jnp.int32),
            pltpu.VMEM((count, width), jnp.float32),
            pltpu.VMEM((count, width), jnp.float32),
            dma, dma((2 * PIECES,)), dma,
        ],
        input_output_aliases={0: 0},
        compiler_params=pltpu.CompilerParams(vmem_limit_bytes=32 << 20),
        name="update",
    )(moved, pair_acc, got, got_ids)
    return new_weights[None, None], new_accum[None, None]


def solution(mesh):
    placed = (
        P("half", "grp", None, None, None),
        P("half", "grp", None, None),
        P(("half", "grp"), None, None, None),
        P(("half", "grp"), None, None),
        P(("half", "grp"), None),
    )
    return jax.shard_map(
        functools.partial(per_device, mesh.shape["half"], mesh.shape["grp"]),
        mesh=mesh,
        in_specs=placed,
        out_specs=(P("half", "grp", None, None, None), P("half", "grp", None, None)),
        check_vma=False,
    )
```

```python
import functools
import math

import jax
import jax.numpy as jnp
from jax import lax
from jax.experimental import pallas as pl
from jax.experimental.pallas import tpu as pltpu
from jax.sharding import PartitionSpec as P

LEARN_RATE = 0.5
EPSILON = 1e-06
LANES = 128
MESH = pl.DeviceIdType.MESH
PIECES = 4
BATCH = 32


def axes_of(groups):
    first = 4 if groups % 4 == 0 else groups
    rest = groups // first
    side = math.isqrt(rest)
    return (first, side, side) if side * side == rest else (first, rest, 1)


def exchange_kernel(
    halves, groups, weights, accum, grads, ids_t, counts,
    table, state, got, got_ids,
    pair_acc, block_buf, id_in, count_in, id_pad, id_buf,
    local_sem, row_send, row_recv, acc_send, acc_recv, block_send, block_recv, id_send, id_recv, ready,
):
    half = lax.axis_index("half")
    group = lax.axis_index("grp")
    owners = halves * groups
    me = half * groups + group
    other = 1 - half
    slots = ids_t.shape[0]
    rows_half = weights.shape[1]
    piece = rows_half // PIECES
    home = pl.multiple_of(half * rows_half, rows_half)

    size_a, size_b, size_c = axes_of(groups)
    at_a = group // (size_b * size_c)
    at_b = lax.rem(group // size_c, size_b)
    at_c = lax.rem(group, size_c)

    def box(low, high, act):
        @pl.loop(low[0], high[0])
        def _(a):
            @pl.loop(low[1], high[1])
            def _(b):
                @pl.loop(low[2], high[2])
                def _(c):
                    peer_group = (a * size_b + b) * size_c + c

                    @pl.when(peer_group != group)
                    def _():
                        act(peer_group, (a, b, c))

    here = (at_a, at_b, at_c)
    past = (at_a + 1, at_b + 1, at_c + 1)

    def descendants(act):
        box(here, (size_a, size_b, size_c), act)

    def ancestors(act):
        box((0, 0, 0), past, act)

    barrier = pltpu.get_barrier_semaphore()
    pl.semaphore_signal(barrier, inc=1, device_id=(other, group), device_id_type=MESH)
    id_load = pltpu.make_async_copy(ids_t, id_in, local_sem.at[1])
    count_load = pltpu.make_async_copy(counts, count_in, local_sem.at[2])
    load = pltpu.make_async_copy(grads, block_buf, local_sem.at[0])
    keep = pltpu.make_async_copy(
        weights.at[half], table.at[pl.ds(home, rows_half)], local_sem.at[3])
    keep_acc = pltpu.make_async_copy(accum, pair_acc.at[half], local_sem.at[4])
    id_load.start()
    count_load.start()
    load.start()

    def greet(peer_group, _):
        for peer_half in range(halves):
            pl.semaphore_signal(barrier, inc=1, device_id=(peer_half, peer_group), device_id_type=MESH)

    descendants(greet)
    id_load.wait()
    count_load.wait()
    slot = lax.broadcasted_iota(jnp.int32, ids_t.shape, 0)
    spare = 2 * rows_half
    id_pad[0:slots, 0:owners] = jnp.where(slot < count_in[...], id_in[...], spare)
    turned = id_pad[...].T
    for owner in range(owners):
        id_buf[owner, 0:1, :] = turned[owner:owner + 1, :]
    load.wait()
    pl.semaphore_wait(barrier, halves * past[0] * past[1] * past[2] - 1)

    def announce(peer_group, _):
        for peer_half in range(halves):
            pl.semaphore_signal(
                ready.at[group], inc=1, device_id=(peer_half, peer_group), device_id_type=MESH)

    ancestors(announce)

    def block_copy(peer_half, peer_group):
        return pltpu.make_async_remote_copy(
            src_ref=block_buf.at[peer_half * groups + peer_group], dst_ref=got.at[me],
            send_sem=block_send, recv_sem=block_recv,
            device_id=(peer_half, peer_group), device_id_type=MESH)

    def id_copy(peer_half, peer_group):
        return pltpu.make_async_remote_copy(
            src_ref=id_buf.at[peer_half * groups + peer_group], dst_ref=got_ids.at[me],
            send_sem=id_send, recv_sem=id_recv,
            device_id=(peer_half, peer_group), device_id_type=MESH)

    def send_ids(peer_group, _):
        for peer_half in range(halves):
            id_copy(peer_half, peer_group).start()

    def send_block(peer_group, _):
        for peer_half in range(halves):
            block_copy(peer_half, peer_group).start()

    def row_copy(index):
        rows = pl.ds(index * piece, piece)
        return pltpu.make_async_remote_copy(
            src_ref=weights.at[other, rows],
            dst_ref=table.at[pl.ds(pl.multiple_of(home + index * piece, piece), piece)],
            send_sem=row_send.at[index], recv_sem=row_recv.at[index],
            device_id=(other, group), device_id_type=MESH)

    acc_copy = pltpu.make_async_remote_copy(
        src_ref=accum, dst_ref=pair_acc.at[half], send_sem=acc_send, recv_sem=acc_recv,
        device_id=(other, group), device_id_type=MESH)
    acc_copy.start()
    for index in range(PIECES):
        row_copy(index).start()
    ancestors(send_ids)
    ancestors(send_block)
    id_copy(other, group).start()
    block_copy(other, group).start()
    keep.start()
    keep_acc.start()

    def serve(joined_group, point):
        pl.semaphore_wait(ready.at[joined_group], halves)
        low = tuple(jnp.where(at > mine, at, 0) for at, mine in zip(point, here))
        high = tuple(at + 1 for at in point)

        def send(peer_group, _):
            send_ids(peer_group, None)
            send_block(peer_group, None)

        box(low, high, send)

    descendants(serve)
    got[me] = block_buf[me]
    got_ids[me] = id_buf[me]

    def take(semaphore, ref):
        pltpu.make_async_copy(ref, ref, semaphore).wait()

    blocks = block_buf.at[pl.ds(0, owners - 1)]
    lists = id_buf.at[pl.ds(0, owners - 1)]
    take(id_send, lists)
    take(block_send, blocks)
    acc_copy.wait()
    keep_acc.wait()
    acc_rows = rows_half // LANES
    for old in range(2):
        line = jnp.where(half == 0, pair_acc[old, 0:1, :], pair_acc[old, 1:2, :])
        for row in range(acc_rows):
            at = old * acc_rows + row
            state[at:at + 1, :] = line[:, row * LANES:(row + 1) * LANES]
    for index in range(PIECES):
        row_copy(index).wait()
    keep.wait()
    take(id_recv, lists)
    take(block_recv, blocks)


def thirds(value):
    first = value.astype(jnp.bfloat16)
    rest = value - first.astype(jnp.float32)
    second = rest.astype(jnp.bfloat16)
    third = (rest - second.astype(jnp.float32)).astype(jnp.bfloat16)
    return jnp.concatenate([first, second, third], axis=1)


def joined(value, width):
    return value[:, 0:width] + value[:, width:2 * width] + value[:, 2 * width:3 * width]


def update_kernel(
    table_in, old_state, got, got_ids, table, new_weights, new_accum,
    out_acc, id_list, delta, acc_sem, out_sem, id_sem,
):
    senders, slots, width = got.shape
    count = senders * slots
    acc_rows = old_state.shape[0] // 2
    rows_half = acc_rows * LANES
    piece = rows_half // PIECES
    spare = 2 * rows_half

    ids_in = pltpu.make_async_copy(got_ids, id_list, id_sem)
    ids_in.start()
    table[spare:spare + 8, :] = jnp.zeros((8, width), jnp.float32)

    lane = lax.broadcasted_iota(jnp.int32, (count, LANES), 1)
    sub = lax.broadcasted_iota(jnp.int32, (count, LANES), 0)
    spread = jnp.broadcast_to(got_ids[...], (senders, slots, LANES)).reshape(count, LANES)
    mine = jnp.where(lane == lax.rem(sub, slots), spread, 0).astype(jnp.float32)
    column = jnp.sum(mine, axis=1, keepdims=True)
    wide = jnp.broadcast_to(column, (count, LANES))
    line = wide.T[0:1, :]
    grad_parts = thirds(got[...].reshape(count, width))
    state_parts = thirds(old_state[...])
    block = min(count, 512)
    tall = lax.broadcasted_iota(jnp.int32, (block, 2 * acc_rows), 1).astype(jnp.float32)
    lane_f = lane[:block].astype(jnp.float32)
    kept = []
    for start in range(0, count, block):
        key = column[start:start + block]
        hot = jnp.where(key == line, 1.0, 0.0)
        total = joined(jnp.dot(hot.astype(jnp.bfloat16), grad_parts,
                               preferred_element_type=jnp.float32), width)
        at_col = lax.broadcasted_iota(jnp.int32, (block, count), 1)
        at_row = lax.broadcasted_iota(jnp.int32, (block, count), 0) + start
        before = jnp.where(at_col < at_row // BATCH * BATCH, hot, 0.0)
        beside = jnp.where((at_col < at_row) & (at_col >= at_row // BATCH * BATCH), hot, 0.0)
        before = jnp.sum(before, axis=1, keepdims=True)
        high = jnp.floor(key * (1.0 / LANES))
        low = key - high * LANES
        row_hot = jnp.where(tall == high, 1.0, 0.0).astype(jnp.bfloat16)
        state_rows = joined(jnp.dot(row_hot, state_parts, preferred_element_type=jnp.float32), LANES)
        at_low = lane_f == low
        old_acc = jnp.sum(jnp.where(at_low, state_rows, 0.0), axis=1, keepdims=True)
        square = jnp.sum(total * total, axis=1, keepdims=True) * (1.0 / width)
        step = LEARN_RATE * total / (jnp.sqrt(old_acc + square) + EPSILON)
        delta[start:start + block, :] = jnp.where(before == 0.0, step, 0.0)
        kept.append((square, before, beside, at_low))
    ids_in.wait()

    @pl.loop(0, count // BATCH)
    def _(batch):
        base = pl.multiple_of(batch * BATCH, BATCH)
        places = [id_list[batch * (BATCH // slots) + at // slots, 0, at % slots] for at in range(BATCH)]
        rows = [table[pl.ds(places[at], 1), :] - delta[pl.ds(base + at, 1), :] for at in range(BATCH)]
        for at in range(BATCH):
            table[pl.ds(places[at], 1), :] = rows[at]

    stores = []
    for old in range(2):
        for index in range(PIECES):
            stores.append(pltpu.make_async_copy(
                table.at[pl.ds(old * rows_half + index * piece, piece)],
                new_weights.at[old, pl.ds(index * piece, piece)],
                out_sem.at[old * PIECES + index]))
    for store in stores:
        store.start()

    gain = jnp.zeros((2 * acc_rows, 3 * LANES), jnp.float32)
    high_line = jnp.floor(line * (1.0 / LANES))
    for index, (square, before, beside, at_low) in enumerate(kept):
        start = index * block
        earlier = before + jnp.sum(beside, axis=1, keepdims=True)
        once = jnp.where(earlier == 0.0, square, 0.0)
        add_parts = thirds(jnp.where(at_low, once, 0.0))
        down = lax.broadcasted_iota(jnp.int32, (2 * acc_rows, block), 0).astype(jnp.float32)
        tall_hot = jnp.where(down == high_line[:, start:start + block], 1.0, 0.0).astype(jnp.bfloat16)
        gain = gain + jnp.dot(tall_hot, add_parts, preferred_element_type=jnp.float32)
    new_state = old_state[...] + joined(gain, LANES)
    for old in range(2):
        for row in range(acc_rows):
            at = old * acc_rows + row
            out_acc[old:old + 1, row * LANES:(row + 1) * LANES] = new_state[at:at + 1, :]
    acc_out = pltpu.make_async_copy(out_acc, new_accum, acc_sem)
    acc_out.start()
    for store in stores:
        store.wait()
    acc_out.wait()


def per_device(halves, groups, weights, accum, grads, row_ids, counts):
    owners, slots, width = grads.shape[1:]
    rows_half = weights.shape[3]
    table = weights[0, 0]
    count = owners * slots
    hbm = pl.BlockSpec(memory_space=pltpu.HBM)
    vmem = pl.BlockSpec(memory_space=pltpu.VMEM)
    id_width = -(-owners // LANES) * LANES
    dma = pltpu.SemaphoreType.DMA
    landed = (
        jax.ShapeDtypeStruct((2 * rows_half + 8, width), jnp.float32),
        jax.ShapeDtypeStruct((2 * rows_half // LANES, LANES), jnp.float32),
        jax.ShapeDtypeStruct((owners, slots, width), jnp.float32),
        jax.ShapeDtypeStruct((owners, 1, LANES), jnp.int32),
    )
    moved, state, got, got_ids = pl.pallas_call(
        functools.partial(exchange_kernel, halves, groups),
        out_shape=landed,
        in_specs=[hbm] * 5,
        out_specs=(vmem,) * 4,
        scratch_shapes=[
            pltpu.VMEM((2, 2, rows_half), jnp.float32),
            pltpu.VMEM((owners, slots, width), jnp.float32),
            pltpu.VMEM((slots, owners), jnp.int32),
            pltpu.VMEM((1, owners), jnp.int32),
            pltpu.VMEM((LANES, id_width), jnp.int32),
            pltpu.VMEM((owners, 1, LANES), jnp.int32),
            dma((5,)),
            dma((PIECES,)), dma((PIECES,)),
            dma, dma,
            dma, dma, dma, dma,
            pltpu.SemaphoreType.REGULAR((groups,)),
        ],
        compiler_params=pltpu.CompilerParams(
            collective_id=0, has_side_effects=True, vmem_limit_bytes=16 << 20),
        name="exchange",
    )(*(pltpu.with_memory_space_constraint(value, pltpu.HBM)
        for value in (table, accum[0, 0], grads[0], row_ids[0].T, counts)))
    _, new_weights, new_accum = pl.pallas_call(
        update_kernel,
        out_shape=(
            jax.ShapeDtypeStruct((2 * rows_half + 8, width), jnp.float32),
            jax.ShapeDtypeStruct((2, rows_half, width), jnp.float32),
            jax.ShapeDtypeStruct((2, rows_half), jnp.float32),
        ),
        in_specs=[vmem] * 4,
        out_specs=(vmem, hbm, hbm),
        scratch_shapes=[
            pltpu.VMEM((2, rows_half), jnp.float32),
            pltpu.SMEM((owners, 1, LANES), jnp.int32),
            pltpu.VMEM((count, width), jnp.float32),
            dma, dma((2 * PIECES,)), dma,
        ],
        input_output_aliases={0: 0},
        compiler_params=pltpu.CompilerParams(vmem_limit_bytes=32 << 20),
        name="update",
    )(moved, state, got, got_ids)
    return new_weights[None, None], new_accum[None, None]


def solution(mesh):
    placed = (
        P("half", "grp", None, None, None),
        P("half", "grp", None, None),
        P(("half", "grp"), None, None, None),
        P(("half", "grp"), None, None),
        P(("half", "grp"), None),
    )
    return jax.shard_map(
        functools.partial(per_device, mesh.shape["half"], mesh.shape["grp"]),
        mesh=mesh,
        in_specs=placed,
        out_specs=(P("half", "grp", None, None, None), P("half", "grp", None, None)),
        check_vma=False,
    )
```

```python
import functools
import math

import jax
import jax.numpy as jnp
from jax import lax
from jax.experimental import pallas as pl
from jax.experimental.pallas import tpu as pltpu
from jax.sharding import PartitionSpec as P

LEARN_RATE = 0.5
EPSILON = 1e-06
LANES = 128
MESH = pl.DeviceIdType.MESH
PIECES = 4
GROUP = 16


def axes_of(groups):
    first = 4 if groups % 4 == 0 else groups
    rest = groups // first
    side = math.isqrt(rest)
    return (first, side, side) if side * side == rest else (first, rest, 1)


def exchange_kernel(
    halves, groups, weights, accum, grads, ids_t, counts,
    table, state, got, got_ids,
    pair_acc, block_buf, id_in, count_in, id_pad, id_buf,
    local_sem, row_send, row_recv, acc_send, acc_recv, block_send, block_recv, id_send, id_recv, ready,
):
    half = lax.axis_index("half")
    group = lax.axis_index("grp")
    owners = halves * groups
    me = half * groups + group
    other = 1 - half
    slots = ids_t.shape[0]
    rows_half = weights.shape[1]
    piece = rows_half // PIECES
    home = pl.multiple_of(half * rows_half, rows_half)

    size_a, size_b, size_c = axes_of(groups)
    at_a = group // (size_b * size_c)
    at_b = lax.rem(group // size_c, size_b)
    at_c = lax.rem(group, size_c)

    def box(low, high, act):
        @pl.loop(low[0], high[0])
        def _(a):
            @pl.loop(low[1], high[1])
            def _(b):
                @pl.loop(low[2], high[2])
                def _(c):
                    peer_group = (a * size_b + b) * size_c + c

                    @pl.when(peer_group != group)
                    def _():
                        act(peer_group, (a, b, c))

    here = (at_a, at_b, at_c)
    past = (at_a + 1, at_b + 1, at_c + 1)

    def descendants(act):
        box(here, (size_a, size_b, size_c), act)

    def ancestors(act):
        box((0, 0, 0), past, act)

    barrier = pltpu.get_barrier_semaphore()
    pl.semaphore_signal(barrier, inc=1, device_id=(other, group), device_id_type=MESH)
    id_load = pltpu.make_async_copy(ids_t, id_in, local_sem.at[1])
    count_load = pltpu.make_async_copy(counts, count_in, local_sem.at[2])
    load = pltpu.make_async_copy(grads, block_buf, local_sem.at[0])
    keep = pltpu.make_async_copy(
        weights.at[half], table.at[pl.ds(home, rows_half)], local_sem.at[3])
    keep_acc = pltpu.make_async_copy(accum, pair_acc.at[half], local_sem.at[4])
    id_load.start()
    count_load.start()
    load.start()

    def greet(peer_group, _):
        for peer_half in range(halves):
            pl.semaphore_signal(barrier, inc=1, device_id=(peer_half, peer_group), device_id_type=MESH)

    descendants(greet)
    pl.semaphore_wait(barrier, halves * past[0] * past[1] * past[2] - 1)

    def announce(peer_group, _):
        for peer_half in range(halves):
            pl.semaphore_signal(
                ready.at[group], inc=1, device_id=(peer_half, peer_group), device_id_type=MESH)

    ancestors(announce)

    def block_copy(peer_half, peer_group):
        return pltpu.make_async_remote_copy(
            src_ref=block_buf.at[peer_half * groups + peer_group], dst_ref=got.at[me],
            send_sem=block_send, recv_sem=block_recv,
            device_id=(peer_half, peer_group), device_id_type=MESH)

    def id_copy(peer_half, peer_group):
        return pltpu.make_async_remote_copy(
            src_ref=id_buf.at[peer_half * groups + peer_group], dst_ref=got_ids.at[me],
            send_sem=id_send, recv_sem=id_recv,
            device_id=(peer_half, peer_group), device_id_type=MESH)

    def send(peer_group, _):
        for peer_half in range(halves):
            id_copy(peer_half, peer_group).start()
            block_copy(peer_half, peer_group).start()

    def row_copy(index):
        rows = pl.ds(index * piece, piece)
        return pltpu.make_async_remote_copy(
            src_ref=weights.at[other, rows],
            dst_ref=table.at[pl.ds(pl.multiple_of(home + index * piece, piece), piece)],
            send_sem=row_send.at[index], recv_sem=row_recv.at[index],
            device_id=(other, group), device_id_type=MESH)

    acc_copy = pltpu.make_async_remote_copy(
        src_ref=accum, dst_ref=pair_acc.at[half], send_sem=acc_send, recv_sem=acc_recv,
        device_id=(other, group), device_id_type=MESH)
    acc_copy.start()
    for index in range(PIECES):
        row_copy(index).start()

    id_load.wait()
    count_load.wait()
    slot = lax.broadcasted_iota(jnp.int32, ids_t.shape, 0)
    spare = 2 * rows_half
    id_pad[0:slots, 0:owners] = jnp.where(slot < count_in[...], id_in[...], spare)
    turned = id_pad[...].T
    for owner in range(owners):
        id_buf[owner, 0:1, :] = turned[owner:owner + 1, :]
    load.wait()
    ancestors(send)
    id_copy(other, group).start()
    block_copy(other, group).start()
    keep.start()
    keep_acc.start()

    def serve(joined_group, point):
        pl.semaphore_wait(ready.at[joined_group], halves)
        low = tuple(jnp.where(at > mine, at, 0) for at, mine in zip(point, here))
        high = tuple(at + 1 for at in point)
        box(low, high, send)

    descendants(serve)
    got[me] = block_buf[me]
    got_ids[me] = id_buf[me]

    def take(semaphore, ref):
        pltpu.make_async_copy(ref, ref, semaphore).wait()

    blocks = block_buf.at[pl.ds(0, owners - 1)]
    lists = id_buf.at[pl.ds(0, owners - 1)]
    take(id_send, lists)
    take(block_send, blocks)
    acc_copy.wait()
    keep_acc.wait()
    acc_rows = rows_half // LANES
    for old in range(2):
        line = jnp.where(half == 0, pair_acc[old, 0:1, :], pair_acc[old, 1:2, :])
        for row in range(acc_rows):
            at = old * acc_rows + row
            state[at:at + 1, :] = line[:, row * LANES:(row + 1) * LANES]
    for index in range(PIECES):
        row_copy(index).wait()
    keep.wait()
    take(id_recv, lists)
    take(block_recv, blocks)


def thirds(value):
    first = value.astype(jnp.bfloat16)
    rest = value - first.astype(jnp.float32)
    second = rest.astype(jnp.bfloat16)
    third = (rest - second.astype(jnp.float32)).astype(jnp.bfloat16)
    return jnp.concatenate([first, second, third], axis=1)


def joined(value, width):
    return value[:, 0:width] + value[:, width:2 * width] + value[:, 2 * width:3 * width]


def update_kernel(
    table_in, old_state, got, got_ids, table, new_weights, new_accum,
    out_acc, id_list, picked, column_kept, square_kept, acc_sem, out_sem, id_sem,
):
    senders, slots, width = got.shape
    count = senders * slots
    acc_rows = old_state.shape[0] // 2
    rows_half = acc_rows * LANES
    piece = rows_half // PIECES
    spare = 2 * rows_half
    block = min(count, 512)

    ids_in = pltpu.make_async_copy(got_ids, id_list, id_sem)
    ids_in.start()
    table[spare:spare + 8, :] = jnp.zeros((8, width), jnp.float32)

    lane = lax.broadcasted_iota(jnp.int32, (count, LANES), 1)
    sub = lax.broadcasted_iota(jnp.int32, (count, LANES), 0)
    spread = jnp.broadcast_to(got_ids[...], (senders, slots, LANES)).reshape(count, LANES)
    mine = jnp.where(lane == lax.rem(sub, slots), spread, 0).astype(jnp.float32)
    column = jnp.sum(mine, axis=1, keepdims=True)
    wide = jnp.broadcast_to(column, (count, LANES))
    column_kept[...] = wide
    line = wide.T[0:1, :]
    grad_parts = thirds(got[...].reshape(count, width))
    state_parts = thirds(old_state[...])
    tall = lax.broadcasted_iota(jnp.int32, (block, 2 * acc_rows), 1).astype(jnp.float32)
    lane_f = lane[:block].astype(jnp.float32)

    def each_row(start, act):
        for at in range(0, block, GROUP):
            sender = (start + at) // slots
            act(start + at, [id_list[sender + index // slots, 0, index % slots] for index in range(GROUP)])

    def gather(base, places):
        rows = [table[pl.ds(place, 1), :] for place in places]
        for index, row in enumerate(rows):
            picked[pl.ds(base + index, 1), :] = row

    def scatter(base, places):
        rows = [picked[pl.ds(base + index, 1), :] for index in range(GROUP)]
        for place, row in zip(places, rows):
            table[pl.ds(place, 1), :] = row

    def over_blocks(act):
        if count == block:
            each_row(0, act)
        else:
            @pl.loop(0, count // block)
            def _(index):
                each_row(index * block, act)

    sums = []
    for start in range(0, count, block):
        key = column[start:start + block]
        hot = jnp.where(key == line, 1.0, 0.0).astype(jnp.bfloat16)
        total = joined(jnp.dot(hot, grad_parts, preferred_element_type=jnp.float32), width)
        high = jnp.floor(key * (1.0 / LANES))
        low = key - high * LANES
        row_hot = jnp.where(tall == high, 1.0, 0.0).astype(jnp.bfloat16)
        state_rows = joined(jnp.dot(row_hot, state_parts, preferred_element_type=jnp.float32), LANES)
        sums.append((total, jnp.where(lane_f == low, state_rows, 0.0)))

    ids_in.wait()
    over_blocks(gather)
    for index, (total, state_rows) in enumerate(sums):
        start = index * block
        old_acc = jnp.sum(state_rows, axis=1, keepdims=True)
        square = jnp.sum(total * total, axis=1, keepdims=True) * (1.0 / width)
        square_kept[start:start + block, :] = jnp.broadcast_to(square, (block, LANES))
        step = LEARN_RATE * total / (jnp.sqrt(old_acc + square) + EPSILON)
        picked[start:start + block, :] = picked[start:start + block, :] - step

    over_blocks(scatter)

    stores = []
    for old in range(2):
        for index in range(PIECES):
            stores.append(pltpu.make_async_copy(
                table.at[pl.ds(old * rows_half + index * piece, piece)],
                new_weights.at[old, pl.ds(index * piece, piece)],
                out_sem.at[old * PIECES + index]))
    for store in stores:
        store.start()
    acc_out = pltpu.make_async_copy(out_acc, new_accum, acc_sem)

    @pl.when(lax.axis_index("half") >= 0)
    def _():
        keys = column_kept[...]
        across = keys.T[0:1, :]
        high_line = jnp.floor(across * (1.0 / LANES))
        gain = jnp.zeros((2 * acc_rows, 3 * LANES), jnp.float32)
        for start in range(0, count, block):
            key = keys[start:start + block, 0:1]
            at_col = lax.broadcasted_iota(jnp.int32, (block, count), 1)
            at_row = lax.broadcasted_iota(jnp.int32, (block, count), 0) + start
            earlier = jnp.sum(
                jnp.where((at_col < at_row) & (key == across), 1.0, 0.0), axis=1, keepdims=True)
            low = keys[start:start + block] - jnp.floor(keys[start:start + block] * (1.0 / LANES)) * LANES
            once = jnp.where((lane_f == low) & (earlier == 0.0), square_kept[start:start + block, :], 0.0)
            add_parts = thirds(once)
            down = lax.broadcasted_iota(jnp.int32, (2 * acc_rows, block), 0).astype(jnp.float32)
            tall_hot = jnp.where(down == high_line[:, start:start + block], 1.0, 0.0).astype(jnp.bfloat16)
            gain = gain + jnp.dot(tall_hot, add_parts, preferred_element_type=jnp.float32)
        new_state = old_state[...] + joined(gain, LANES)
        for old in range(2):
            for row in range(acc_rows):
                at = old * acc_rows + row
                out_acc[old:old + 1, row * LANES:(row + 1) * LANES] = new_state[at:at + 1, :]

    acc_out.start()
    for store in stores:
        store.wait()
    acc_out.wait()


def per_device(halves, groups, weights, accum, grads, row_ids, counts):
    owners, slots, width = grads.shape[1:]
    rows_half = weights.shape[3]
    table = weights[0, 0]
    count = owners * slots
    hbm = pl.BlockSpec(memory_space=pltpu.HBM)
    vmem = pl.BlockSpec(memory_space=pltpu.VMEM)
    id_width = -(-owners // LANES) * LANES
    dma = pltpu.SemaphoreType.DMA
    landed = (
        jax.ShapeDtypeStruct((2 * rows_half + 8, width), jnp.float32),
        jax.ShapeDtypeStruct((2 * rows_half // LANES, LANES), jnp.float32),
        jax.ShapeDtypeStruct((owners, slots, width), jnp.float32),
        jax.ShapeDtypeStruct((owners, 1, LANES), jnp.int32),
    )
    moved, state, got, got_ids = pl.pallas_call(
        functools.partial(exchange_kernel, halves, groups),
        out_shape=landed,
        in_specs=[hbm] * 5,
        out_specs=(vmem,) * 4,
        scratch_shapes=[
            pltpu.VMEM((2, 2, rows_half), jnp.float32),
            pltpu.VMEM((owners, slots, width), jnp.float32),
            pltpu.VMEM((slots, owners), jnp.int32),
            pltpu.VMEM((1, owners), jnp.int32),
            pltpu.VMEM((LANES, id_width), jnp.int32),
            pltpu.VMEM((owners, 1, LANES), jnp.int32),
            dma((5,)),
            dma((PIECES,)), dma((PIECES,)),
            dma, dma,
            dma, dma, dma, dma,
            pltpu.SemaphoreType.REGULAR((groups,)),
        ],
        compiler_params=pltpu.CompilerParams(
            collective_id=0, has_side_effects=True, vmem_limit_bytes=16 << 20),
        name="exchange",
    )(*(pltpu.with_memory_space_constraint(value, pltpu.HBM)
        for value in (table, accum[0, 0], grads[0], row_ids[0].T, counts)))
    _, new_weights, new_accum = pl.pallas_call(
        update_kernel,
        out_shape=(
            jax.ShapeDtypeStruct((2 * rows_half + 8, width), jnp.float32),
            jax.ShapeDtypeStruct((2, rows_half, width), jnp.float32),
            jax.ShapeDtypeStruct((2, rows_half), jnp.float32),
        ),
        in_specs=[vmem] * 4,
        out_specs=(vmem, hbm, hbm),
        scratch_shapes=[
            pltpu.VMEM((2, rows_half), jnp.float32),
            pltpu.SMEM((owners, 1, LANES), jnp.int32),
            pltpu.VMEM((count, width), jnp.float32),
            pltpu.VMEM((count, LANES), jnp.float32),
            pltpu.VMEM((count, LANES), jnp.float32),
            dma, dma((2 * PIECES,)), dma,
        ],
        input_output_aliases={0: 0},
        compiler_params=pltpu.CompilerParams(vmem_limit_bytes=32 << 20),
        name="update",
    )(moved, state, got, got_ids)
    return new_weights[None, None], new_accum[None, None]


def solution(mesh):
    placed = (
        P("half", "grp", None, None, None),
        P("half", "grp", None, None),
        P(("half", "grp"), None, None, None),
        P(("half", "grp"), None, None),
        P(("half", "grp"), None),
    )
    return jax.shard_map(
        functools.partial(per_device, mesh.shape["half"], mesh.shape["grp"]),
        mesh=mesh,
        in_specs=placed,
        out_specs=(P("half", "grp", None, None, None), P("half", "grp", None, None)),
        check_vma=False,
    )
```

```python
import functools
import math

import jax
import jax.numpy as jnp
from jax import lax
from jax.experimental import pallas as pl
from jax.experimental.pallas import tpu as pltpu
from jax.sharding import PartitionSpec as P

LEARN_RATE = 0.5
EPSILON = 1e-06
LANES = 128
MESH = pl.DeviceIdType.MESH
PIECES = 4
GROUP = 16


def axes_of(groups):
    first = 4 if groups % 4 == 0 else groups
    rest = groups // first
    side = math.isqrt(rest)
    return (first, side, side) if side * side == rest else (first, rest, 1)


def exchange_kernel(
    halves, groups, weights, accum, grads, ids_t, counts,
    table, state, got, got_ids,
    pair_acc, block_buf, id_in, count_in, id_pad, id_buf,
    local_sem, row_send, row_recv, acc_send, acc_recv, block_send, block_recv, id_send, id_recv, ready,
):
    half = lax.axis_index("half")
    group = lax.axis_index("grp")
    owners = halves * groups
    me = half * groups + group
    other = 1 - half
    slots = ids_t.shape[0]
    rows_half = weights.shape[1]
    piece = rows_half // PIECES
    home = pl.multiple_of(half * rows_half, rows_half)

    size_a, size_b, size_c = axes_of(groups)
    at_a = group // (size_b * size_c)
    at_b = lax.rem(group // size_c, size_b)
    at_c = lax.rem(group, size_c)

    def box(low, high, act):
        @pl.loop(low[0], high[0])
        def _(a):
            @pl.loop(low[1], high[1])
            def _(b):
                @pl.loop(low[2], high[2])
                def _(c):
                    peer_group = (a * size_b + b) * size_c + c

                    @pl.when(peer_group != group)
                    def _():
                        act(peer_group, (a, b, c))

    here = (at_a, at_b, at_c)
    past = (at_a + 1, at_b + 1, at_c + 1)

    def descendants(act):
        box(here, (size_a, size_b, size_c), act)

    def ancestors(act):
        box((0, 0, 0), past, act)

    barrier = pltpu.get_barrier_semaphore()
    pl.semaphore_signal(barrier, inc=1, device_id=(other, group), device_id_type=MESH)
    id_load = pltpu.make_async_copy(ids_t, id_in, local_sem.at[1])
    count_load = pltpu.make_async_copy(counts, count_in, local_sem.at[2])
    load = pltpu.make_async_copy(grads, block_buf, local_sem.at[0])
    keep = pltpu.make_async_copy(
        weights.at[half], table.at[pl.ds(home, rows_half)], local_sem.at[3])
    keep_acc = pltpu.make_async_copy(accum, pair_acc.at[half], local_sem.at[4])
    id_load.start()
    count_load.start()
    load.start()

    def greet(peer_group, _):
        for peer_half in range(halves):
            pl.semaphore_signal(barrier, inc=1, device_id=(peer_half, peer_group), device_id_type=MESH)

    descendants(greet)
    pl.semaphore_wait(barrier, halves * past[0] * past[1] * past[2] - 1)

    def announce(peer_group, _):
        for peer_half in range(halves):
            pl.semaphore_signal(
                ready.at[group], inc=1, device_id=(peer_half, peer_group), device_id_type=MESH)

    ancestors(announce)

    def block_copy(peer_half, peer_group):
        return pltpu.make_async_remote_copy(
            src_ref=block_buf.at[peer_half * groups + peer_group], dst_ref=got.at[me],
            send_sem=block_send, recv_sem=block_recv,
            device_id=(peer_half, peer_group), device_id_type=MESH)

    def id_copy(peer_half, peer_group):
        return pltpu.make_async_remote_copy(
            src_ref=id_buf.at[peer_half * groups + peer_group], dst_ref=got_ids.at[me],
            send_sem=id_send, recv_sem=id_recv,
            device_id=(peer_half, peer_group), device_id_type=MESH)

    def send(peer_group, _):
        for turn in range(halves):
            peer_half = lax.rem(half + turn + 1, halves)
            block_copy(peer_half, peer_group).start()
            id_copy(peer_half, peer_group).start()

    def row_copy(index):
        rows = pl.ds(index * piece, piece)
        return pltpu.make_async_remote_copy(
            src_ref=weights.at[other, rows],
            dst_ref=table.at[pl.ds(pl.multiple_of(home + index * piece, piece), piece)],
            send_sem=row_send.at[index], recv_sem=row_recv.at[index],
            device_id=(other, group), device_id_type=MESH)

    acc_copy = pltpu.make_async_remote_copy(
        src_ref=accum, dst_ref=pair_acc.at[half], send_sem=acc_send, recv_sem=acc_recv,
        device_id=(other, group), device_id_type=MESH)
    acc_copy.start()
    for index in range(PIECES):
        row_copy(index).start()

    id_load.wait()
    count_load.wait()
    slot = lax.broadcasted_iota(jnp.int32, ids_t.shape, 0)
    spare = 2 * rows_half
    id_pad[0:slots, 0:owners] = jnp.where(slot < count_in[...], id_in[...], spare)
    turned = id_pad[...].T
    for owner in range(owners):
        id_buf[owner, 0:1, :] = turned[owner:owner + 1, :]
    load.wait()
    def wave(act):
        @pl.loop(0, at_a + at_b + at_c)
        def _(distance):
            @pl.loop(0, past[1])
            def _(b):
                @pl.loop(0, past[2])
                def _(c):
                    a = distance - b - c

                    @pl.when((a >= 0) & (a <= at_a))
                    def _():
                        act((a * size_b + b) * size_c + c, (a, b, c))

    wave(send)
    id_copy(other, group).start()
    block_copy(other, group).start()
    keep.start()
    keep_acc.start()

    def serve(joined_group, point):
        pl.semaphore_wait(ready.at[joined_group], halves)
        low = tuple(jnp.where(at > mine, at, 0) for at, mine in zip(point, here))
        high = tuple(at + 1 for at in point)
        box(low, high, send)

    @pl.loop(1, size_a + size_b + size_c - at_a - at_b - at_c - 2)
    def _(distance):
        @pl.loop(at_b, size_b)
        def _(b):
            @pl.loop(at_c, size_c)
            def _(c):
                a = at_a + distance - (b - at_b) - (c - at_c)

                @pl.when((a >= at_a) & (a < size_a))
                def _():
                    serve((a * size_b + b) * size_c + c, (a, b, c))

    got[me] = block_buf[me]
    got_ids[me] = id_buf[me]

    def take(semaphore, ref):
        pltpu.make_async_copy(ref, ref, semaphore).wait()

    blocks = block_buf.at[pl.ds(0, owners - 1)]
    lists = id_buf.at[pl.ds(0, owners - 1)]
    take(id_send, lists)
    take(block_send, blocks)
    acc_copy.wait()
    keep_acc.wait()
    acc_rows = rows_half // LANES
    for old in range(2):
        line = jnp.where(half == 0, pair_acc[old, 0:1, :], pair_acc[old, 1:2, :])
        for row in range(acc_rows):
            at = old * acc_rows + row
            state[at:at + 1, :] = line[:, row * LANES:(row + 1) * LANES]
    for index in range(PIECES):
        row_copy(index).wait()
    keep.wait()
    take(id_recv, lists)
    take(block_recv, blocks)


def thirds(value):
    first = value.astype(jnp.bfloat16)
    rest = value - first.astype(jnp.float32)
    second = rest.astype(jnp.bfloat16)
    third = (rest - second.astype(jnp.float32)).astype(jnp.bfloat16)
    return jnp.concatenate([first, second, third], axis=1)


def joined(value, width):
    return value[:, 0:width] + value[:, width:2 * width] + value[:, 2 * width:3 * width]


def update_kernel(
    table_in, old_state, got, got_ids, table, new_weights, new_accum,
    out_acc, id_list, picked, column_kept, square_kept, acc_sem, out_sem, id_sem,
):
    senders, slots, width = got.shape
    count = senders * slots
    acc_rows = old_state.shape[0] // 2
    rows_half = acc_rows * LANES
    piece = rows_half // PIECES
    spare = 2 * rows_half
    block = min(count, 512)

    part = senders // 2
    ids_in = [
        pltpu.make_async_copy(got_ids.at[pl.ds(at, part)], id_list.at[pl.ds(at, part)], id_sem.at[at // part])
        for at in (0, part)]
    for copy in ids_in:
        copy.start()
    table[spare:spare + 8, :] = jnp.zeros((8, width), jnp.float32)

    lane = lax.broadcasted_iota(jnp.int32, (count, LANES), 1)
    sub = lax.broadcasted_iota(jnp.int32, (count, LANES), 0)
    spread = jnp.broadcast_to(got_ids[...], (senders, slots, LANES)).reshape(count, LANES)
    mine = jnp.where(lane == lax.rem(sub, slots), spread, 0).astype(jnp.float32)
    column = jnp.sum(mine, axis=1, keepdims=True)
    wide = jnp.broadcast_to(column, (count, LANES))
    column_kept[...] = wide
    line = wide.T[0:1, :]
    grad_parts = thirds(got[...].reshape(count, width))
    state_parts = thirds(old_state[...])
    tall = lax.broadcasted_iota(jnp.int32, (block, 2 * acc_rows), 1).astype(jnp.float32)
    lane_f = lane[:block].astype(jnp.float32)

    def each_row(start, length, act):
        for at in range(0, length, GROUP):
            sender = (start + at) // slots
            act(start + at, [id_list[sender + index // slots, 0, index % slots] for index in range(GROUP)])

    def gather(base, places):
        rows = [table[pl.ds(place, 1), :] for place in places]
        for index, row in enumerate(rows):
            picked[pl.ds(base + index, 1), :] = row

    def scatter(base, places):
        rows = [picked[pl.ds(base + index, 1), :] for index in range(GROUP)]
        for place, row in zip(places, rows):
            table[pl.ds(place, 1), :] = row

    def over_blocks(act):
        if count == block:
            each_row(0, block, act)
        else:
            @pl.loop(0, count // block)
            def _(index):
                each_row(index * block, block, act)

    sums = []
    for start in range(0, count, block):
        key = column[start:start + block]
        hot = jnp.where(key == line, 1.0, 0.0).astype(jnp.bfloat16)
        total = joined(jnp.dot(hot, grad_parts, preferred_element_type=jnp.float32), width)
        high = jnp.floor(key * (1.0 / LANES))
        low = key - high * LANES
        row_hot = jnp.where(tall == high, 1.0, 0.0).astype(jnp.bfloat16)
        state_rows = joined(jnp.dot(row_hot, state_parts, preferred_element_type=jnp.float32), LANES)
        sums.append((total, jnp.where(lane_f == low, state_rows, 0.0)))

    if count == block:
        ids_in[0].wait()
        each_row(0, block // 2, gather)
        ids_in[1].wait()
        each_row(block // 2, block // 2, gather)
    else:
        for copy in ids_in:
            copy.wait()
        over_blocks(gather)
    for index, (total, state_rows) in enumerate(sums):
        start = index * block
        old_acc = jnp.sum(state_rows, axis=1, keepdims=True)
        square = jnp.sum(total * total, axis=1, keepdims=True) * (1.0 / width)
        square_kept[start:start + block, :] = jnp.broadcast_to(square, (block, LANES))
        step = LEARN_RATE * total / (jnp.sqrt(old_acc + square) + EPSILON)
        picked[start:start + block, :] = picked[start:start + block, :] - step

    over_blocks(scatter)

    stores = []
    for old in range(2):
        for index in range(PIECES):
            stores.append(pltpu.make_async_copy(
                table.at[pl.ds(old * rows_half + index * piece, piece)],
                new_weights.at[old, pl.ds(index * piece, piece)],
                out_sem.at[old * PIECES + index]))
    for store in stores:
        store.start()
    acc_out = pltpu.make_async_copy(out_acc, new_accum, acc_sem)

    @pl.when(lax.axis_index("half") >= 0)
    def _():
        keys = column_kept[...]
        across = keys.T[0:1, :]
        high_line = jnp.floor(across * (1.0 / LANES))
        gain = jnp.zeros((2 * acc_rows, 3 * LANES), jnp.float32)
        for start in range(0, count, block):
            key = keys[start:start + block, 0:1]
            at_col = lax.broadcasted_iota(jnp.int32, (block, count), 1)
            at_row = lax.broadcasted_iota(jnp.int32, (block, count), 0) + start
            earlier = jnp.sum(
                jnp.where((at_col < at_row) & (key == across), 1.0, 0.0), axis=1, keepdims=True)
            low = keys[start:start + block] - jnp.floor(keys[start:start + block] * (1.0 / LANES)) * LANES
            once = jnp.where((lane_f == low) & (earlier == 0.0), square_kept[start:start + block, :], 0.0)
            add_parts = thirds(once)
            down = lax.broadcasted_iota(jnp.int32, (2 * acc_rows, block), 0).astype(jnp.float32)
            tall_hot = jnp.where(down == high_line[:, start:start + block], 1.0, 0.0).astype(jnp.bfloat16)
            gain = gain + jnp.dot(tall_hot, add_parts, preferred_element_type=jnp.float32)
        new_state = old_state[...] + joined(gain, LANES)
        for old in range(2):
            for row in range(acc_rows):
                at = old * acc_rows + row
                out_acc[old:old + 1, row * LANES:(row + 1) * LANES] = new_state[at:at + 1, :]

    acc_out.start()
    for store in stores:
        store.wait()
    acc_out.wait()


def per_device(halves, groups, weights, accum, grads, row_ids, counts):
    owners, slots, width = grads.shape[1:]
    rows_half = weights.shape[3]
    table = weights[0, 0]
    count = owners * slots
    hbm = pl.BlockSpec(memory_space=pltpu.HBM)
    vmem = pl.BlockSpec(memory_space=pltpu.VMEM)
    id_width = -(-owners // LANES) * LANES
    dma = pltpu.SemaphoreType.DMA
    landed = (
        jax.ShapeDtypeStruct((2 * rows_half + 8, width), jnp.float32),
        jax.ShapeDtypeStruct((2 * rows_half // LANES, LANES), jnp.float32),
        jax.ShapeDtypeStruct((owners, slots, width), jnp.float32),
        jax.ShapeDtypeStruct((owners, 1, LANES), jnp.int32),
    )
    moved, state, got, got_ids = pl.pallas_call(
        functools.partial(exchange_kernel, halves, groups),
        out_shape=landed,
        in_specs=[hbm] * 5,
        out_specs=(vmem,) * 4,
        scratch_shapes=[
            pltpu.VMEM((2, 2, rows_half), jnp.float32),
            pltpu.VMEM((owners, slots, width), jnp.float32),
            pltpu.VMEM((slots, owners), jnp.int32),
            pltpu.VMEM((1, owners), jnp.int32),
            pltpu.VMEM((LANES, id_width), jnp.int32),
            pltpu.VMEM((owners, 1, LANES), jnp.int32),
            dma((5,)),
            dma((PIECES,)), dma((PIECES,)),
            dma, dma,
            dma, dma, dma, dma,
            pltpu.SemaphoreType.REGULAR((groups,)),
        ],
        compiler_params=pltpu.CompilerParams(
            collective_id=0, has_side_effects=True, vmem_limit_bytes=16 << 20),
        name="exchange",
    )(*(pltpu.with_memory_space_constraint(value, pltpu.HBM)
        for value in (table, accum[0, 0], grads[0], row_ids[0].T, counts)))
    _, new_weights, new_accum = pl.pallas_call(
        update_kernel,
        out_shape=(
            jax.ShapeDtypeStruct((2 * rows_half + 8, width), jnp.float32),
            jax.ShapeDtypeStruct((2, rows_half, width), jnp.float32),
            jax.ShapeDtypeStruct((2, rows_half), jnp.float32),
        ),
        in_specs=[vmem] * 4,
        out_specs=(vmem, hbm, hbm),
        scratch_shapes=[
            pltpu.VMEM((2, rows_half), jnp.float32),
            pltpu.SMEM((owners, 1, LANES), jnp.int32),
            pltpu.VMEM((count, width), jnp.float32),
            pltpu.VMEM((count, LANES), jnp.float32),
            pltpu.VMEM((count, LANES), jnp.float32),
            dma, dma((2 * PIECES,)), dma((2,)),
        ],
        input_output_aliases={0: 0},
        compiler_params=pltpu.CompilerParams(vmem_limit_bytes=32 << 20),
        name="update",
    )(moved, state, got, got_ids)
    return new_weights[None, None], new_accum[None, None]


def solution(mesh):
    placed = (
        P("half", "grp", None, None, None),
        P("half", "grp", None, None),
        P(("half", "grp"), None, None, None),
        P(("half", "grp"), None, None),
        P(("half", "grp"), None),
    )
    return jax.shard_map(
        functools.partial(per_device, mesh.shape["half"], mesh.shape["grp"]),
        mesh=mesh,
        in_specs=placed,
        out_specs=(P("half", "grp", None, None, None), P("half", "grp", None, None)),
        check_vma=False,
    )
```

```python
import functools
import math

import jax
import jax.numpy as jnp
from jax import lax
from jax.experimental import pallas as pl
from jax.experimental.pallas import tpu as pltpu
from jax.sharding import PartitionSpec as P

LEARN_RATE = 0.5
EPSILON = 1e-06
LANES = 128
MESH = pl.DeviceIdType.MESH
PIECES = 4
GROUP = 16


def axes_of(groups):
    first = 4 if groups % 4 == 0 else groups
    rest = groups // first
    side = math.isqrt(rest)
    return (first, side, side) if side * side == rest else (first, rest, 1)


def exchange_kernel(
    halves, groups, weights, accum, grads, ids_t, counts,
    table, state, got, column_kept, lines,
    got_ids, pair_acc, block_buf, id_in, count_in, id_pad, id_buf,
    local_sem, row_send, row_recv, acc_send, acc_recv, block_send, block_recv, id_send, id_recv, ready,
):
    half = lax.axis_index("half")
    group = lax.axis_index("grp")
    owners = halves * groups
    me = half * groups + group
    other = 1 - half
    slots = ids_t.shape[0]
    rows_half = weights.shape[1]
    piece = rows_half // PIECES
    home = pl.multiple_of(half * rows_half, rows_half)

    size_a, size_b, size_c = axes_of(groups)
    at_a = group // (size_b * size_c)
    at_b = lax.rem(group // size_c, size_b)
    at_c = lax.rem(group, size_c)

    def box(low, high, act):
        @pl.loop(low[0], high[0])
        def _(a):
            @pl.loop(low[1], high[1])
            def _(b):
                @pl.loop(low[2], high[2])
                def _(c):
                    peer_group = (a * size_b + b) * size_c + c

                    @pl.when(peer_group != group)
                    def _():
                        act(peer_group, (a, b, c))

    here = (at_a, at_b, at_c)
    past = (at_a + 1, at_b + 1, at_c + 1)

    def descendants(act):
        box(here, (size_a, size_b, size_c), act)

    def ancestors(act):
        box((0, 0, 0), past, act)

    barrier = pltpu.get_barrier_semaphore()
    pl.semaphore_signal(barrier, inc=1, device_id=(other, group), device_id_type=MESH)
    id_load = pltpu.make_async_copy(ids_t, id_in, local_sem.at[1])
    count_load = pltpu.make_async_copy(counts, count_in, local_sem.at[2])
    load = pltpu.make_async_copy(grads, block_buf, local_sem.at[0])
    keep = pltpu.make_async_copy(
        weights.at[half], table.at[pl.ds(home, rows_half)], local_sem.at[3])
    keep_acc = pltpu.make_async_copy(accum, pair_acc.at[half], local_sem.at[4])
    id_load.start()
    count_load.start()
    load.start()

    def greet(peer_group, _):
        for peer_half in range(halves):
            pl.semaphore_signal(barrier, inc=1, device_id=(peer_half, peer_group), device_id_type=MESH)

    descendants(greet)
    pl.semaphore_wait(barrier, halves * past[0] * past[1] * past[2] - 1)

    def announce(peer_group, _):
        for peer_half in range(halves):
            pl.semaphore_signal(
                ready.at[group], inc=1, device_id=(peer_half, peer_group), device_id_type=MESH)

    ancestors(announce)

    def block_copy(peer_half, peer_group):
        return pltpu.make_async_remote_copy(
            src_ref=block_buf.at[peer_half * groups + peer_group], dst_ref=got.at[me],
            send_sem=block_send, recv_sem=block_recv,
            device_id=(peer_half, peer_group), device_id_type=MESH)

    def id_copy(peer_half, peer_group):
        return pltpu.make_async_remote_copy(
            src_ref=id_buf.at[peer_half * groups + peer_group], dst_ref=got_ids.at[me],
            send_sem=id_send, recv_sem=id_recv,
            device_id=(peer_half, peer_group), device_id_type=MESH)

    def send_ids(peer_group, _):
        for turn in range(halves):
            id_copy(lax.rem(half + turn + 1, halves), peer_group).start()

    def send_block(peer_group, _):
        for turn in range(halves):
            block_copy(lax.rem(half + turn + 1, halves), peer_group).start()

    def row_copy(index):
        rows = pl.ds(index * piece, piece)
        return pltpu.make_async_remote_copy(
            src_ref=weights.at[other, rows],
            dst_ref=table.at[pl.ds(pl.multiple_of(home + index * piece, piece), piece)],
            send_sem=row_send.at[index], recv_sem=row_recv.at[index],
            device_id=(other, group), device_id_type=MESH)

    acc_copy = pltpu.make_async_remote_copy(
        src_ref=accum, dst_ref=pair_acc.at[half], send_sem=acc_send, recv_sem=acc_recv,
        device_id=(other, group), device_id_type=MESH)
    acc_copy.start()
    for index in range(PIECES):
        row_copy(index).start()

    id_load.wait()
    count_load.wait()
    slot = lax.broadcasted_iota(jnp.int32, ids_t.shape, 0)
    spare = 2 * rows_half
    id_pad[0:slots, 0:owners] = jnp.where(slot < count_in[...], id_in[...], spare)
    turned = id_pad[...].T
    for owner in range(owners):
        id_buf[owner, 0:1, :] = turned[owner:owner + 1, :]
    load.wait()
    def wave(act):
        @pl.loop(0, at_a + at_b + at_c)
        def _(distance):
            @pl.loop(0, past[1])
            def _(b):
                @pl.loop(0, past[2])
                def _(c):
                    a = distance - b - c

                    @pl.when((a >= 0) & (a <= at_a))
                    def _():
                        act((a * size_b + b) * size_c + c, (a, b, c))

    wave(send_ids)
    wave(send_block)
    id_copy(other, group).start()
    block_copy(other, group).start()
    keep.start()
    keep_acc.start()

    def serve(joined_group, point):
        pl.semaphore_wait(ready.at[joined_group], halves)
        low = tuple(jnp.where(at > mine, at, 0) for at, mine in zip(point, here))
        high = tuple(at + 1 for at in point)
        box(low, high, send_ids)
        box(low, high, send_block)

    @pl.loop(1, size_a + size_b + size_c - at_a - at_b - at_c - 2)
    def _(distance):
        @pl.loop(at_b, size_b)
        def _(b):
            @pl.loop(at_c, size_c)
            def _(c):
                a = at_a + distance - (b - at_b) - (c - at_c)

                @pl.when((a >= at_a) & (a < size_a))
                def _():
                    serve((a * size_b + b) * size_c + c, (a, b, c))

    got[me] = block_buf[me]
    got_ids[me] = id_buf[me]

    def take(semaphore, ref):
        pltpu.make_async_copy(ref, ref, semaphore).wait()

    blocks = block_buf.at[pl.ds(0, owners - 1)]
    lists = id_buf.at[pl.ds(0, owners - 1)]
    acc_copy.wait()
    keep_acc.wait()
    acc_rows = rows_half // LANES
    for old in range(2):
        line = jnp.where(half == 0, pair_acc[old, 0:1, :], pair_acc[old, 1:2, :])
        for row in range(acc_rows):
            at = old * acc_rows + row
            state[at:at + 1, :] = line[:, row * LANES:(row + 1) * LANES]
    take(id_recv, lists)
    count = owners * slots
    lane = lax.broadcasted_iota(jnp.int32, (count, LANES), 1)
    sub = lax.broadcasted_iota(jnp.int32, (count, LANES), 0)
    spread = jnp.broadcast_to(got_ids[...], (owners, slots, LANES)).reshape(count, LANES)
    mine = jnp.where(lane == lax.rem(sub, slots), spread, 0).astype(jnp.float32)
    wide = jnp.broadcast_to(jnp.sum(mine, axis=1, keepdims=True), (count, LANES))
    column_kept[...] = wide
    line = wide.T[0:1, :].astype(jnp.int32)
    for row in range(count // LANES):
        lines[row:row + 1, :] = line[:, row * LANES:(row + 1) * LANES]
    for index in range(PIECES):
        row_copy(index).wait()
    keep.wait()
    take(id_send, lists)
    take(block_recv, blocks)
    take(block_send, blocks)


def thirds(value):
    first = value.astype(jnp.bfloat16)
    rest = value - first.astype(jnp.float32)
    second = rest.astype(jnp.bfloat16)
    third = (rest - second.astype(jnp.float32)).astype(jnp.bfloat16)
    return jnp.concatenate([first, second, third], axis=1)


def joined(value, width):
    return value[:, 0:width] + value[:, width:2 * width] + value[:, 2 * width:3 * width]


def update_kernel(
    table_in, old_state, got, column_kept, lines, table, new_weights, new_accum,
    out_acc, id_list, picked, square_kept, acc_sem, out_sem, id_sem,
):
    senders, slots, width = got.shape
    count = senders * slots
    acc_rows = old_state.shape[0] // 2
    rows_half = acc_rows * LANES
    piece = rows_half // PIECES
    spare = 2 * rows_half
    block = min(count, 512)

    ids_in = pltpu.make_async_copy(lines, id_list, id_sem)
    ids_in.start()
    table[spare:spare + 8, :] = jnp.zeros((8, width), jnp.float32)

    lane = lax.broadcasted_iota(jnp.int32, (block, LANES), 1)
    line = jnp.concatenate([lines[row:row + 1, :] for row in range(count // LANES)], axis=1).astype(jnp.float32)
    grad_parts = thirds(got[...].reshape(count, width))
    state_parts = thirds(old_state[...])
    tall = lax.broadcasted_iota(jnp.int32, (block, 2 * acc_rows), 1).astype(jnp.float32)
    lane_f = lane.astype(jnp.float32)

    def each_row(start, length, act):
        for at in range(0, length, GROUP):
            act(start + at, [id_list[start // LANES + (at + index) // LANES, (at + index) % LANES] for index in range(GROUP)])

    def gather(base, places):
        rows = [table[pl.ds(place, 1), :] for place in places]
        for index, row in enumerate(rows):
            picked[pl.ds(base + index, 1), :] = row

    def scatter(base, places):
        rows = [picked[pl.ds(base + index, 1), :] for index in range(GROUP)]
        for place, row in zip(places, rows):
            table[pl.ds(place, 1), :] = row

    def over_blocks(act):
        if count == block:
            each_row(0, block, act)
        else:
            @pl.loop(0, count // block)
            def _(index):
                each_row(index * block, block, act)

    sums = []
    for start in range(0, count, block):
        key = column_kept[start:start + block, 0:1]
        hot = jnp.where(key == line, 1.0, 0.0).astype(jnp.bfloat16)
        total = joined(jnp.dot(hot, grad_parts, preferred_element_type=jnp.float32), width)
        high = jnp.floor(key * (1.0 / LANES))
        low = key - high * LANES
        row_hot = jnp.where(tall == high, 1.0, 0.0).astype(jnp.bfloat16)
        state_rows = joined(jnp.dot(row_hot, state_parts, preferred_element_type=jnp.float32), LANES)
        sums.append((total, jnp.where(lane_f == low, state_rows, 0.0)))

    ids_in.wait()
    over_blocks(gather)
    for index, (total, state_rows) in enumerate(sums):
        start = index * block
        old_acc = jnp.sum(state_rows, axis=1, keepdims=True)
        square = jnp.sum(total * total, axis=1, keepdims=True) * (1.0 / width)
        square_kept[start:start + block, :] = jnp.broadcast_to(square, (block, LANES))
        step = LEARN_RATE * total / (jnp.sqrt(old_acc + square) + EPSILON)
        picked[start:start + block, :] = picked[start:start + block, :] - step

    over_blocks(scatter)

    stores = []
    for old in range(2):
        for index in range(PIECES):
            stores.append(pltpu.make_async_copy(
                table.at[pl.ds(old * rows_half + index * piece, piece)],
                new_weights.at[old, pl.ds(index * piece, piece)],
                out_sem.at[old * PIECES + index]))
    for store in stores:
        store.start()
    acc_out = pltpu.make_async_copy(out_acc, new_accum, acc_sem)

    @pl.when(lax.axis_index("half") >= 0)
    def _():
        keys = column_kept[...]
        across = keys.T[0:1, :]
        high_line = jnp.floor(across * (1.0 / LANES))
        gain = jnp.zeros((2 * acc_rows, 3 * LANES), jnp.float32)
        for start in range(0, count, block):
            key = keys[start:start + block, 0:1]
            at_col = lax.broadcasted_iota(jnp.int32, (block, count), 1)
            at_row = lax.broadcasted_iota(jnp.int32, (block, count), 0) + start
            earlier = jnp.sum(
                jnp.where((at_col < at_row) & (key == across), 1.0, 0.0), axis=1, keepdims=True)
            low = keys[start:start + block] - jnp.floor(keys[start:start + block] * (1.0 / LANES)) * LANES
            once = jnp.where((lane_f == low) & (earlier == 0.0), square_kept[start:start + block, :], 0.0)
            add_parts = thirds(once)
            down = lax.broadcasted_iota(jnp.int32, (2 * acc_rows, block), 0).astype(jnp.float32)
            tall_hot = jnp.where(down == high_line[:, start:start + block], 1.0, 0.0).astype(jnp.bfloat16)
            gain = gain + jnp.dot(tall_hot, add_parts, preferred_element_type=jnp.float32)
        new_state = old_state[...] + joined(gain, LANES)
        for old in range(2):
            for row in range(acc_rows):
                at = old * acc_rows + row
                out_acc[old:old + 1, row * LANES:(row + 1) * LANES] = new_state[at:at + 1, :]

    acc_out.start()
    for store in stores:
        store.wait()
    acc_out.wait()


def per_device(halves, groups, weights, accum, grads, row_ids, counts):
    owners, slots, width = grads.shape[1:]
    rows_half = weights.shape[3]
    table = weights[0, 0]
    count = owners * slots
    hbm = pl.BlockSpec(memory_space=pltpu.HBM)
    vmem = pl.BlockSpec(memory_space=pltpu.VMEM)
    id_width = -(-owners // LANES) * LANES
    dma = pltpu.SemaphoreType.DMA
    landed = (
        jax.ShapeDtypeStruct((2 * rows_half + 8, width), jnp.float32),
        jax.ShapeDtypeStruct((2 * rows_half // LANES, LANES), jnp.float32),
        jax.ShapeDtypeStruct((owners, slots, width), jnp.float32),
        jax.ShapeDtypeStruct((count, LANES), jnp.float32),
        jax.ShapeDtypeStruct((count // LANES, LANES), jnp.int32),
    )
    moved, state, got, column, lines = pl.pallas_call(
        functools.partial(exchange_kernel, halves, groups),
        out_shape=landed,
        in_specs=[hbm] * 5,
        out_specs=(vmem,) * 5,
        scratch_shapes=[
            pltpu.VMEM((owners, 1, LANES), jnp.int32),
            pltpu.VMEM((2, 2, rows_half), jnp.float32),
            pltpu.VMEM((owners, slots, width), jnp.float32),
            pltpu.VMEM((slots, owners), jnp.int32),
            pltpu.VMEM((1, owners), jnp.int32),
            pltpu.VMEM((LANES, id_width), jnp.int32),
            pltpu.VMEM((owners, 1, LANES), jnp.int32),
            dma((5,)),
            dma((PIECES,)), dma((PIECES,)),
            dma, dma,
            dma, dma, dma, dma,
            pltpu.SemaphoreType.REGULAR((groups,)),
        ],
        compiler_params=pltpu.CompilerParams(
            collective_id=0, has_side_effects=True, vmem_limit_bytes=16 << 20),
        name="exchange",
    )(*(pltpu.with_memory_space_constraint(value, pltpu.HBM)
        for value in (table, accum[0, 0], grads[0], row_ids[0].T, counts)))
    _, new_weights, new_accum = pl.pallas_call(
        update_kernel,
        out_shape=(
            jax.ShapeDtypeStruct((2 * rows_half + 8, width), jnp.float32),
            jax.ShapeDtypeStruct((2, rows_half, width), jnp.float32),
            jax.ShapeDtypeStruct((2, rows_half), jnp.float32),
        ),
        in_specs=[vmem] * 5,
        out_specs=(vmem, hbm, hbm),
        scratch_shapes=[
            pltpu.VMEM((2, rows_half), jnp.float32),
            pltpu.SMEM((count // LANES, LANES), jnp.int32),
            pltpu.VMEM((count, width), jnp.float32),
            pltpu.VMEM((count, LANES), jnp.float32),
            dma, dma((2 * PIECES,)), dma,
        ],
        input_output_aliases={0: 0},
        compiler_params=pltpu.CompilerParams(vmem_limit_bytes=32 << 20),
        name="update",
    )(moved, state, got, column, lines)
    return new_weights[None, None], new_accum[None, None]


def solution(mesh):
    placed = (
        P("half", "grp", None, None, None),
        P("half", "grp", None, None),
        P(("half", "grp"), None, None, None),
        P(("half", "grp"), None, None),
        P(("half", "grp"), None),
    )
    return jax.shard_map(
        functools.partial(per_device, mesh.shape["half"], mesh.shape["grp"]),
        mesh=mesh,
        in_specs=placed,
        out_specs=(P("half", "grp", None, None, None), P("half", "grp", None, None)),
        check_vma=False,
    )
```

```python
import functools
import math

import jax
import jax.numpy as jnp
from jax import lax
from jax.experimental import pallas as pl
from jax.experimental.pallas import tpu as pltpu
from jax.sharding import PartitionSpec as P

LEARN_RATE = 0.5
EPSILON = 1e-06
LANES = 128
MESH = pl.DeviceIdType.MESH
PIECES = 4
WRITES = 2
GROUP = 8


def axes_of(groups):
    first = 4 if groups % 4 == 0 else groups
    rest = groups // first
    side = math.isqrt(rest)
    return (first, side, side) if side * side == rest else (first, rest, 1)


def exchange_kernel(
    halves, groups, weights, accum, grads, ids_t, counts,
    table, state, got, column_kept, lines,
    got_ids, pair_acc, block_buf, id_in, count_in, id_pad, id_buf,
    local_sem, row_send, row_recv, acc_send, acc_recv, block_send, block_recv, id_send, id_recv, ready,
):
    half = lax.axis_index("half")
    group = lax.axis_index("grp")
    owners = halves * groups
    me = half * groups + group
    other = 1 - half
    slots = ids_t.shape[0]
    rows_half = weights.shape[1]
    piece = rows_half // PIECES
    home = pl.multiple_of(half * rows_half, rows_half)

    size_a, size_b, size_c = axes_of(groups)
    at_a = group // (size_b * size_c)
    at_b = lax.rem(group // size_c, size_b)
    at_c = lax.rem(group, size_c)

    def box(low, high, act):
        @pl.loop(low[0], high[0])
        def _(a):
            @pl.loop(low[1], high[1])
            def _(b):
                @pl.loop(low[2], high[2])
                def _(c):
                    peer_group = (a * size_b + b) * size_c + c

                    @pl.when(peer_group != group)
                    def _():
                        act(peer_group, (a, b, c))

    here = (at_a, at_b, at_c)
    past = (at_a + 1, at_b + 1, at_c + 1)

    def descendants(act):
        box(here, (size_a, size_b, size_c), act)

    def ancestors(act):
        box((0, 0, 0), past, act)

    barrier = pltpu.get_barrier_semaphore()
    pl.semaphore_signal(barrier, inc=1, device_id=(other, group), device_id_type=MESH)
    id_load = pltpu.make_async_copy(ids_t, id_in, local_sem.at[1])
    count_load = pltpu.make_async_copy(counts, count_in, local_sem.at[2])
    load = pltpu.make_async_copy(grads, block_buf, local_sem.at[0])
    keep = pltpu.make_async_copy(
        weights.at[half], table.at[pl.ds(home, rows_half)], local_sem.at[3])
    keep_acc = pltpu.make_async_copy(accum, pair_acc.at[half], local_sem.at[4])
    id_load.start()
    count_load.start()
    load.start()

    def greet(peer_group, _):
        for peer_half in range(halves):
            pl.semaphore_signal(barrier, inc=1, device_id=(peer_half, peer_group), device_id_type=MESH)

    descendants(greet)
    pl.semaphore_wait(barrier, halves * past[0] * past[1] * past[2] - 1)

    def announce(peer_group, _):
        for peer_half in range(halves):
            pl.semaphore_signal(
                ready.at[group], inc=1, device_id=(peer_half, peer_group), device_id_type=MESH)

    ancestors(announce)

    def block_copy(peer_half, peer_group):
        return pltpu.make_async_remote_copy(
            src_ref=block_buf.at[peer_half * groups + peer_group], dst_ref=got.at[me],
            send_sem=block_send, recv_sem=block_recv,
            device_id=(peer_half, peer_group), device_id_type=MESH)

    def id_copy(peer_half, peer_group):
        return pltpu.make_async_remote_copy(
            src_ref=id_buf.at[peer_half * groups + peer_group], dst_ref=got_ids.at[me],
            send_sem=id_send, recv_sem=id_recv,
            device_id=(peer_half, peer_group), device_id_type=MESH)

    def send_ids(peer_group, _):
        for turn in range(halves):
            id_copy(lax.rem(half + turn + 1, halves), peer_group).start()

    def send_block(peer_group, _):
        for turn in range(halves):
            block_copy(lax.rem(half + turn + 1, halves), peer_group).start()

    def row_copy(index):
        rows = pl.ds(index * piece, piece)
        return pltpu.make_async_remote_copy(
            src_ref=weights.at[other, rows],
            dst_ref=table.at[pl.ds(pl.multiple_of(home + index * piece, piece), piece)],
            send_sem=row_send.at[index], recv_sem=row_recv.at[index],
            device_id=(other, group), device_id_type=MESH)

    acc_copy = pltpu.make_async_remote_copy(
        src_ref=accum, dst_ref=pair_acc.at[half], send_sem=acc_send, recv_sem=acc_recv,
        device_id=(other, group), device_id_type=MESH)
    acc_copy.start()
    for index in range(PIECES):
        row_copy(index).start()

    id_load.wait()
    count_load.wait()
    slot = lax.broadcasted_iota(jnp.int32, ids_t.shape, 0)
    spare = 2 * rows_half
    id_pad[0:slots, 0:owners] = jnp.where(slot < count_in[...], id_in[...], spare)
    turned = id_pad[...].T
    for owner in range(owners):
        id_buf[owner, 0:1, :] = turned[owner:owner + 1, :]
    load.wait()
    def wave(act):
        @pl.loop(0, at_a + at_b + at_c)
        def _(distance):
            @pl.loop(0, past[1])
            def _(b):
                @pl.loop(0, past[2])
                def _(c):
                    a = distance - b - c

                    @pl.when((a >= 0) & (a <= at_a))
                    def _():
                        act((a * size_b + b) * size_c + c, (a, b, c))

    wave(send_ids)
    wave(send_block)
    id_copy(other, group).start()
    block_copy(other, group).start()
    keep.start()
    keep_acc.start()

    def serve(joined_group, point):
        pl.semaphore_wait(ready.at[joined_group], halves)
        low = tuple(jnp.where(at > mine, at, 0) for at, mine in zip(point, here))
        high = tuple(at + 1 for at in point)
        box(low, high, send_ids)
        box(low, high, send_block)

    @pl.loop(1, size_a + size_b + size_c - at_a - at_b - at_c - 2)
    def _(distance):
        @pl.loop(at_b, size_b)
        def _(b):
            @pl.loop(at_c, size_c)
            def _(c):
                a = at_a + distance - (b - at_b) - (c - at_c)

                @pl.when((a >= at_a) & (a < size_a))
                def _():
                    serve((a * size_b + b) * size_c + c, (a, b, c))

    got[me] = block_buf[me]
    got_ids[me] = id_buf[me]

    def take(semaphore, ref):
        pltpu.make_async_copy(ref, ref, semaphore).wait()

    blocks = block_buf.at[pl.ds(0, owners - 1)]
    lists = id_buf.at[pl.ds(0, owners - 1)]
    acc_copy.wait()
    keep_acc.wait()
    acc_rows = rows_half // LANES
    for old in range(2):
        line = jnp.where(half == 0, pair_acc[old, 0:1, :], pair_acc[old, 1:2, :])
        for row in range(acc_rows):
            at = old * acc_rows + row
            state[at:at + 1, :] = line[:, row * LANES:(row + 1) * LANES]
    take(id_recv, lists)
    count = owners * slots
    lane = lax.broadcasted_iota(jnp.int32, (count, LANES), 1)
    sub = lax.broadcasted_iota(jnp.int32, (count, LANES), 0)
    spread = jnp.broadcast_to(got_ids[...], (owners, slots, LANES)).reshape(count, LANES)
    mine = jnp.where(lane == lax.rem(sub, slots), spread, 0).astype(jnp.float32)
    wide = jnp.broadcast_to(jnp.sum(mine, axis=1, keepdims=True), (count, LANES))
    column_kept[...] = wide
    line = wide.T[0:1, :].astype(jnp.int32)
    for row in range(count // LANES):
        lines[row:row + 1, :] = line[:, row * LANES:(row + 1) * LANES]
    for index in range(PIECES):
        row_copy(index).wait()
    keep.wait()
    take(id_send, lists)
    take(block_recv, blocks)
    take(block_send, blocks)


def thirds(value):
    first = value.astype(jnp.bfloat16)
    rest = value - first.astype(jnp.float32)
    second = rest.astype(jnp.bfloat16)
    third = (rest - second.astype(jnp.float32)).astype(jnp.bfloat16)
    return jnp.concatenate([first, second, third], axis=1)


def joined(value, width):
    return value[:, 0:width] + value[:, width:2 * width] + value[:, 2 * width:3 * width]


def update_kernel(
    table_in, old_state, got, column_kept, lines, table, new_weights, new_accum,
    out_acc, id_list, picked, square_kept, acc_sem, out_sem, id_sem,
):
    senders, slots, width = got.shape
    count = senders * slots
    acc_rows = old_state.shape[0] // 2
    rows_half = acc_rows * LANES
    piece = rows_half // WRITES
    spare = 2 * rows_half
    block = min(count, 512)

    ids_in = pltpu.make_async_copy(lines, id_list, id_sem)
    ids_in.start()
    table[spare:spare + 8, :] = jnp.zeros((8, width), jnp.float32)

    lane = lax.broadcasted_iota(jnp.int32, (block, LANES), 1)
    line = jnp.concatenate([lines[row:row + 1, :] for row in range(count // LANES)], axis=1).astype(jnp.float32)
    grad_parts = thirds(got[...].reshape(count, width))
    state_parts = thirds(old_state[...])
    tall = lax.broadcasted_iota(jnp.int32, (block, 2 * acc_rows), 1).astype(jnp.float32)
    lane_f = lane.astype(jnp.float32)

    def each_row(start, length, act):
        for at in range(0, length, GROUP):
            act(start + at, [id_list[start // LANES + (at + index) // LANES, (at + index) % LANES] for index in range(GROUP)])

    def gather(base, places):
        rows = [table[pl.ds(place, 1), :] for place in places]
        for index, row in enumerate(rows):
            picked[pl.ds(base + index, 1), :] = row

    def scatter(base, places):
        rows = [picked[pl.ds(base + index, 1), :] for index in range(GROUP)]
        for place, row in zip(places, rows):
            table[pl.ds(place, 1), :] = row

    def over_blocks(act):
        if count == block:
            each_row(0, block, act)
        else:
            @pl.loop(0, count // block)
            def _(index):
                each_row(index * block, block, act)

    sums = []
    for start in range(0, count, block):
        key = column_kept[start:start + block, 0:1]
        hot = jnp.where(key == line, 1.0, 0.0).astype(jnp.bfloat16)
        total = joined(jnp.dot(hot, grad_parts, preferred_element_type=jnp.float32), width)
        high = jnp.floor(key * (1.0 / LANES))
        low = key - high * LANES
        row_hot = jnp.where(tall == high, 1.0, 0.0).astype(jnp.bfloat16)
        state_rows = joined(jnp.dot(row_hot, state_parts, preferred_element_type=jnp.float32), LANES)
        sums.append((total, jnp.where(lane_f == low, state_rows, 0.0)))

    ids_in.wait()
    over_blocks(gather)
    for index, (total, state_rows) in enumerate(sums):
        start = index * block
        old_acc = jnp.sum(state_rows, axis=1, keepdims=True)
        square = jnp.sum(total * total, axis=1, keepdims=True) * (1.0 / width)
        square_kept[start:start + block, :] = jnp.broadcast_to(square, (block, LANES))
        step = LEARN_RATE * total / (jnp.sqrt(old_acc + square) + EPSILON)
        picked[start:start + block, :] = picked[start:start + block, :] - step

    over_blocks(scatter)

    stores = []
    for old in range(2):
        for index in range(WRITES):
            stores.append(pltpu.make_async_copy(
                table.at[pl.ds(old * rows_half + index * piece, piece)],
                new_weights.at[old, pl.ds(index * piece, piece)],
                out_sem.at[old * WRITES + index]))
    for store in stores:
        store.start()
    acc_out = pltpu.make_async_copy(out_acc, new_accum, acc_sem)

    @pl.when(lax.axis_index("half") >= 0)
    def _():
        keys = column_kept[...]
        across = keys.T[0:1, :]
        high_line = jnp.floor(across * (1.0 / LANES))
        gain = jnp.zeros((2 * acc_rows, 3 * LANES), jnp.float32)
        for start in range(0, count, block):
            key = keys[start:start + block, 0:1]
            at_col = lax.broadcasted_iota(jnp.int32, (block, count), 1)
            at_row = lax.broadcasted_iota(jnp.int32, (block, count), 0) + start
            earlier = jnp.sum(
                jnp.where((at_col < at_row) & (key == across), 1.0, 0.0), axis=1, keepdims=True)
            low = keys[start:start + block] - jnp.floor(keys[start:start + block] * (1.0 / LANES)) * LANES
            once = jnp.where((lane_f == low) & (earlier == 0.0), square_kept[start:start + block, :], 0.0)
            add_parts = thirds(once)
            down = lax.broadcasted_iota(jnp.int32, (2 * acc_rows, block), 0).astype(jnp.float32)
            tall_hot = jnp.where(down == high_line[:, start:start + block], 1.0, 0.0).astype(jnp.bfloat16)
            gain = gain + jnp.dot(tall_hot, add_parts, preferred_element_type=jnp.float32)
        new_state = old_state[...] + joined(gain, LANES)
        for old in range(2):
            for row in range(acc_rows):
                at = old * acc_rows + row
                out_acc[old:old + 1, row * LANES:(row + 1) * LANES] = new_state[at:at + 1, :]

    acc_out.start()
    for store in stores:
        store.wait()
    acc_out.wait()


def per_device(halves, groups, weights, accum, grads, row_ids, counts):
    owners, slots, width = grads.shape[1:]
    rows_half = weights.shape[3]
    table = weights[0, 0]
    count = owners * slots
    hbm = pl.BlockSpec(memory_space=pltpu.HBM)
    vmem = pl.BlockSpec(memory_space=pltpu.VMEM)
    id_width = -(-owners // LANES) * LANES
    dma = pltpu.SemaphoreType.DMA
    landed = (
        jax.ShapeDtypeStruct((2 * rows_half + 8, width), jnp.float32),
        jax.ShapeDtypeStruct((2 * rows_half // LANES, LANES), jnp.float32),
        jax.ShapeDtypeStruct((owners, slots, width), jnp.float32),
        jax.ShapeDtypeStruct((count, LANES), jnp.float32),
        jax.ShapeDtypeStruct((count // LANES, LANES), jnp.int32),
    )
    moved, state, got, column, lines = pl.pallas_call(
        functools.partial(exchange_kernel, halves, groups),
        out_shape=landed,
        in_specs=[hbm] * 5,
        out_specs=(vmem,) * 5,
        scratch_shapes=[
            pltpu.VMEM((owners, 1, LANES), jnp.int32),
            pltpu.VMEM((2, 2, rows_half), jnp.float32),
            pltpu.VMEM((owners, slots, width), jnp.float32),
            pltpu.VMEM((slots, owners), jnp.int32),
            pltpu.VMEM((1, owners), jnp.int32),
            pltpu.VMEM((LANES, id_width), jnp.int32),
            pltpu.VMEM((owners, 1, LANES), jnp.int32),
            dma((5,)),
            dma((PIECES,)), dma((PIECES,)),
            dma, dma,
            dma, dma, dma, dma,
            pltpu.SemaphoreType.REGULAR((groups,)),
        ],
        compiler_params=pltpu.CompilerParams(
            collective_id=0, has_side_effects=True, vmem_limit_bytes=16 << 20),
        name="exchange",
    )(*(pltpu.with_memory_space_constraint(value, pltpu.HBM)
        for value in (table, accum[0, 0], grads[0], row_ids[0].T, counts)))
    _, new_weights, new_accum = pl.pallas_call(
        update_kernel,
        out_shape=(
            jax.ShapeDtypeStruct((2 * rows_half + 8, width), jnp.float32),
            jax.ShapeDtypeStruct((2, rows_half, width), jnp.float32),
            jax.ShapeDtypeStruct((2, rows_half), jnp.float32),
        ),
        in_specs=[vmem] * 5,
        out_specs=(vmem, hbm, hbm),
        scratch_shapes=[
            pltpu.VMEM((2, rows_half), jnp.float32),
            pltpu.SMEM((count // LANES, LANES), jnp.int32),
            pltpu.VMEM((count, width), jnp.float32),
            pltpu.VMEM((count, LANES), jnp.float32),
            dma, dma((2 * WRITES,)), dma,
        ],
        input_output_aliases={0: 0},
        compiler_params=pltpu.CompilerParams(vmem_limit_bytes=32 << 20),
        name="update",
    )(moved, state, got, column, lines)
    return new_weights[None, None], new_accum[None, None]


def solution(mesh):
    placed = (
        P("half", "grp", None, None, None),
        P("half", "grp", None, None),
        P(("half", "grp"), None, None, None),
        P(("half", "grp"), None, None),
        P(("half", "grp"), None),
    )
    return jax.shard_map(
        functools.partial(per_device, mesh.shape["half"], mesh.shape["grp"]),
        mesh=mesh,
        in_specs=placed,
        out_specs=(P("half", "grp", None, None, None), P("half", "grp", None, None)),
        check_vma=False,
    )
```
